512 devices in a mesh: seq: 128 (over x, z, core), head: 4 (over y).
Axes of the slice: x: 4, y: 4, z: 16, core: 2. Of those that a mesh axis runs over, the one named last changes fastest.
Arguments:
- queries: bfloat16 [16384, 1024], P('seq', 'head'), may hold values from -6 to 6
- keys: bfloat16 [16384, 1024], P('seq', 'head'), may hold values from -6 to 6
- values: bfloat16 [16384, 1024], P('seq', 'head'), may hold values from -3 to 3
- out_grad: bfloat16 [16384, 1024], P('seq', 'head'), may hold values from -3 to 3
- w_query: bfloat16 [1024, 2048], P('head'), may hold values from -0.1875 to 0.1875
- w_key: bfloat16 [1024, 2048], P('head'), may hold values from -0.1875 to 0.1875
- w_value: bfloat16 [1024, 2048], P('head'), may hold values from -0.1875 to 0.1875
Outputs:
- input_grad: bfloat16 [16384, 2048], P('seq', 'head')
The draws below stay inside these ranges and needn't reach their ends.
All inputs are finite; a program needn't handle non-finite values.
Results may differ from the reference program's by a relative error of at most 0.0064.
Values sent between devices are 32-bit elements; how exact they have to be, the bound alone decides.
No kernel may reach another device: no remote copies, remote signals or barrier semaphores. Data moves between devices by JAX's collectives and lax.ppermute only.
A program may use at most 128 MiB of HBM per device.

```python
import jax
import jax.numpy as jnp
import numpy as np
from jax import lax

HD = 64
HEADS = 16
D = 2048
FEATS = 2080
TOK_DEV = 128
TOKENS = 16384
N_SEQ = 128


def block_scale(own_key, dims, shards, low, top_value):
    def one(dim, parts):
        heights = jax.random.uniform(jax.random.fold_in(jax.random.fold_in(own_key, 6), dim), (parts,), jnp.float32, low / len(shards), top_value / len(shards))
        return jnp.repeat(jnp.exp(heights), dims[dim] // parts).reshape((-1,) + (1,) * (len(dims) - dim - 1))

    loudness = one(*shards[0])
    for cut in shards[1:]:
        loudness = loudness * one(*cut)
    return loudness


def gaussian(own_key, extent, spread, reach, shards=(), kind=jnp.bfloat16):
    values = spread * jax.random.normal(own_key, extent, jnp.float32)
    if shards:
        values = values * block_scale(own_key, extent, shards, -0.22, 0.18)
    return jnp.clip(values, -reach, reach).astype(kind)


def setup_inputs(seed: int = 0) -> dict:
    seeds = jax.random.split(jax.random.key(seed), 8)
    queries = gaussian(seeds[0], (TOKENS, HEADS * HD), 1.0, 6.0, ((0, 128), (1, 4)))
    keys = gaussian(seeds[1], (TOKENS, HEADS * HD), 1.0, 6.0, ((0, 128), (1, 4)))
    values = gaussian(seeds[2], (TOKENS, HEADS * HD), 0.5, 3.0, ((0, 128), (1, 4)))
    out_grad = gaussian(seeds[3], (TOKENS, HEADS * HD), 0.5, 3.0, ((0, 128), (1, 4)))
    w_query = gaussian(seeds[4], (HEADS * HD, D), (HEADS * HD) ** -0.5, 0.1875, ((0, 4),))
    w_key = gaussian(seeds[5], (HEADS * HD, D), (HEADS * HD) ** -0.5, 0.1875, ((0, 4),))
    w_value = gaussian(seeds[6], (HEADS * HD, D), (HEADS * HD) ** -0.5, 0.1875, ((0, 4),))
    return {"queries": queries, "keys": keys, "values": values, "out_grad": out_grad, "w_query": w_query, "w_key": w_key, "w_value": w_value}


def pair_tables(width):
    first, second = np.triu_indices(width)
    count = first.shape[0]
    select_first = np.zeros((width, count), np.float32)
    select_second = np.zeros((width, count), np.float32)
    select_first[first, np.arange(count)] = 1.0
    select_second[second, np.arange(count)] = 1.0
    scaling = np.where(first == second, 1.0, np.sqrt(2.0)) / width
    return (select_first, select_second, scaling.astype(np.float32))

def expand_features(inputs, pick_first, pick_second, scaling):
    first = jnp.dot(inputs, pick_first, preferred_element_type=jnp.float32)
    second = jnp.dot(inputs, pick_second, preferred_element_type=jnp.float32)
    return (first.astype(jnp.bfloat16), second.astype(jnp.bfloat16), (first * second * scaling).astype(jnp.bfloat16))

def chain_back(first, second, dphi, back_first, back_second, scaling):
    left = dphi * scaling * second.astype(jnp.float32)
    right = dphi * scaling * first.astype(jnp.float32)
    return jnp.dot(left, back_first, precision=lax.Precision.HIGHEST, preferred_element_type=jnp.float32) + jnp.dot(right, back_second, precision=lax.Precision.HIGHEST, preferred_element_type=jnp.float32)

def reference(queries, keys, values, out_grad, w_query, w_key, w_value):
    select_first, select_second, scale_np = pair_tables(HD)
    pick_first = jnp.asarray(select_first, jnp.bfloat16)
    pick_second = jnp.asarray(select_second, jnp.bfloat16)
    back_first = jnp.asarray(select_first.T, jnp.float32)
    back_second = jnp.asarray(select_second.T, jnp.float32)
    scaling = jnp.asarray(scale_np, jnp.float32)

    def shaped(array):
        return array.reshape(N_SEQ, TOK_DEV, HEADS, HD)
    blocks = (shaped(queries), shaped(keys), shaped(values), shaped(out_grad))
    zero_state = jnp.zeros((FEATS, HEADS, HD), jnp.float32)

    def features_of(array):
        first, second, feats = expand_features(array.reshape(TOK_DEV * HEADS, HD), pick_first, pick_second, scaling)
        return (first, second, feats)

    def state_of(feats, other):
        return jnp.einsum('thf,thd->fhd', feats.reshape(TOK_DEV, HEADS, FEATS).astype(jnp.float32), other.astype(jnp.float32))

    def total_step(total, block):
        query_b, key_b, value_b, grad_b = block
        feats = features_of(query_b)[2]
        return (total + state_of(feats, grad_b), None)
    grad_total, unused = lax.scan(total_step, zero_state, blocks)
    causal = lax.broadcasted_iota(jnp.int32, (TOK_DEV, TOK_DEV), 0) >= lax.broadcasted_iota(jnp.int32, (TOK_DEV, TOK_DEV), 1)

    def step(carry, block):
        kv_sum, grad_sum = carry
        query_b, key_b, value_b, grad_b = block
        qfirst, qsecond, fq = features_of(query_b)
        kfirst, ksecond, fk = features_of(key_b)
        kv_local = state_of(fk, value_b)
        grad_local = state_of(fq, grad_b)
        kv_before = kv_sum.astype(jnp.bfloat16).astype(jnp.float32)
        grad_after = (grad_total - grad_sum - grad_local).astype(jnp.bfloat16).astype(jnp.float32)
        qf = query_b.astype(jnp.float32)
        kf = key_b.astype(jnp.float32)
        vf = value_b.astype(jnp.float32)
        gf = grad_b.astype(jnp.float32)
        scores = jnp.einsum('thd,shd->hts', qf, kf)
        products = jnp.einsum('thd,shd->hts', gf, vf)
        attn = jnp.where(causal, (scores / HD) ** 2, 0.0).astype(jnp.bfloat16).astype(jnp.float32)
        pgrad = jnp.where(causal, 2.0 * scores * products / (HD * HD), 0.0).astype(jnp.bfloat16).astype(jnp.float32)
        dfq = jnp.einsum('thd,fhd->thf', gf, kv_before).reshape(TOK_DEV * HEADS, FEATS)
        dfk = jnp.einsum('thd,fhd->thf', vf, grad_after).reshape(TOK_DEV * HEADS, FEATS)
        query_grad = jnp.einsum('hts,shd->thd', pgrad, kf) + chain_back(qfirst, qsecond, dfq, back_first, back_second, scaling).reshape(TOK_DEV, HEADS, HD)
        key_grad = jnp.einsum('hts,thd->shd', pgrad, qf) + chain_back(kfirst, ksecond, dfk, back_first, back_second, scaling).reshape(TOK_DEV, HEADS, HD)
        value_grad = jnp.einsum('hts,thd->shd', attn, gf) + jnp.einsum('thf,fhd->thd', fk.reshape(TOK_DEV, HEADS, FEATS).astype(jnp.float32), grad_after)
        mixed = jnp.dot(query_grad.astype(jnp.bfloat16).reshape(TOK_DEV, HEADS * HD), w_query, preferred_element_type=jnp.float32)
        mixed = mixed + jnp.dot(key_grad.astype(jnp.bfloat16).reshape(TOK_DEV, HEADS * HD), w_key, preferred_element_type=jnp.float32)
        mixed = mixed + jnp.dot(value_grad.astype(jnp.bfloat16).reshape(TOK_DEV, HEADS * HD), w_value, preferred_element_type=jnp.float32)
        return ((kv_sum + kv_local, grad_sum + grad_local), mixed.astype(jnp.bfloat16))
    unused_carry, result = lax.scan(step, (zero_state, zero_state), blocks)
    return result.reshape(N_SEQ * TOK_DEV, D)
```

```python
import functools

import jax
import jax.numpy as jnp
from jax import lax
from jax.experimental import pallas as pl
from jax.experimental.pallas import tpu as pltpu
from jax.sharding import Mesh
from jax.sharding import PartitionSpec as P

HD = 64
TB = 128
CHIPS = 4
BLOCKS = 8
GRAIN = 8
SIZES = [HD - GRAIN * (j // GRAIN) for j in range(HD)]
STARTS = [sum(SIZES[:j]) for j in range(HD)]
PAIRS = sum(SIZES)
HALF = PAIRS // 2
SPLIT_J = STARTS.index(HALF)
VMEM = pl.BlockSpec(memory_space=pltpu.VMEM)
F32 = jnp.float32
BF16 = jnp.bfloat16


def call(body, out_shape, args, name, scratch=(), flops=0, nbytes=0):
    return pl.pallas_call(
        body,
        out_shape=out_shape,
        in_specs=[VMEM] * len(args),
        out_specs=jax.tree.map(lambda unused: VMEM, out_shape),
        scratch_shapes=list(scratch),
        name=name,
        compiler_params=pltpu.CompilerParams(vmem_limit_bytes=24 << 20),
        cost_estimate=pl.CostEstimate(flops=flops, bytes_accessed=nbytes, transcendentals=0),
    )(*args)


def dot(a, b):
    return jnp.dot(a, b, preferred_element_type=F32)


def pack_body(q_ref, k_ref, v_ref, g_ref, out_ref):
    for head in range(CHIPS):
        cols = slice(head * HD, (head + 1) * HD)
        out_ref[head, 0] = jnp.concatenate([q_ref[:, cols], g_ref[:, cols]], axis=1).astype(F32)
        out_ref[head, 1] = jnp.concatenate([k_ref[:, cols], v_ref[:, cols]], axis=1).astype(F32)


def write_features(xt, factor, feats_ref):
    for block in range(HD // GRAIN):
        low = GRAIN * block
        base = xt[low:]
        if factor != 1.0 and low + GRAIN < HD:
            base = jnp.concatenate([xt[low : low + GRAIN], xt[low + GRAIN :] * factor], axis=0)
        for j in range(low, low + GRAIN, 2):
            pair = [base * xt[j : j + 1], base * xt[j + 1 : j + 2]]
            start = STARTS[j]
            feats_ref[start : start + 2 * SIZES[j], :] = jnp.concatenate(pair, axis=0).astype(BF16)


def state_body(own_ref, other_ref, state_ref, tok_ref, src_ref, out_ref, feats_ref):
    core = lax.axis_index("core")
    for chip in range(CHIPS):
        for ref, parity in ((own_ref, core), (other_ref, 1 - core)):
            source = ref[chip, 1 - core]
            tok_ref[2 * chip + parity] = source.astype(BF16)
            src_ref[2 * chip + parity] = source.T.astype(BF16)
            out_ref[2 * chip + parity] = ref[chip, core].T.astype(BF16)
    state_ref[...] = jnp.zeros_like(state_ref)

    def step(tile, carry):
        xt = jnp.concatenate([src_ref[2 * tile, :HD], src_ref[2 * tile + 1, :HD]], axis=1)
        write_features(xt.astype(F32), 1.0, feats_ref)
        tok = jnp.concatenate([tok_ref[2 * tile], tok_ref[2 * tile + 1]], axis=0)
        values = tok[:, HD:]
        zeros = jnp.zeros_like(values)
        state_ref[...] += dot(
            feats_ref[:HALF, :], jnp.concatenate([values, zeros], axis=1)
        ) + dot(feats_ref[HALF:, :], jnp.concatenate([zeros, values], axis=1))
        return carry

    lax.fori_loop(0, BLOCKS // 2, step, 0)


def local_body(tok_ref, src_ref, out_ref, local_ref):
    core = lax.axis_index("core")
    tiles = BLOCKS // 2
    width = 2 * TB
    sign = 1 - 2 * core
    local_ref[...] = jnp.zeros_like(local_ref)
    ahead = lax.broadcasted_iota(jnp.int32, (width, width), 0) - lax.broadcasted_iota(
        jnp.int32, (width, width), 1
    )

    def outer(tile, carry):
        target = jnp.concatenate([out_ref[2 * tile], out_ref[2 * tile + 1]], axis=1)
        zeros = jnp.zeros((HD, width), BF16)
        score_rhs = jnp.concatenate([target[:HD], zeros], axis=0)
        value_rhs = jnp.concatenate([zeros, target[HD:]], axis=0)

        def inner(source, carry):
            tok = jnp.concatenate([tok_ref[2 * source], tok_ref[2 * source + 1]], axis=0)
            scores = dot(tok, score_rhs)
            products = dot(tok, value_rhs)
            keep = (ahead + (source - tile) * width) * sign <= 0
            scaled = jnp.where(keep, scores, 0.0) * (1.0 / HD)
            attn = (scaled * scaled).astype(BF16)
            pgrad = (scaled * products * (2.0 / HD)).astype(BF16)
            left = jnp.concatenate([src_ref[2 * source], src_ref[2 * source + 1]], axis=1)
            local_ref[tile, :HD] += dot(left[:HD], pgrad)
            local_ref[tile, HD:] += dot(left[HD:], attn)
            return carry

        first = jnp.where(core == 0, 0, tile)
        last = jnp.where(core == 0, tile + 1, tiles)
        lax.fori_loop(first, last, inner, 0)
        return carry

    lax.fori_loop(0, tiles, outer, 0)


def scan_body(parts_ref, sums_ref):
    core = lax.axis_index("core")
    count = parts_ref.shape[0]

    def step(number, total):
        place = number + core * (count - 1 - 2 * number)
        sums_ref[place] = total
        return total + parts_ref[place]

    lax.fori_loop(0, count, step, jnp.zeros(parts_ref.shape[1:], F32))


def grads_body(state_ref, out_ref, local_ref, grads_ref, rows_ref, cols_ref, wide_ref, feats_ref):
    rows_ref[...] = state_ref[...].astype(BF16)
    for tile in range(HALF // TB):
        part = slice(tile * TB, (tile + 1) * TB)
        cols_ref[:, part] = state_ref[part, :].T.astype(BF16)

    def step(tile, carry):
        target = jnp.concatenate([out_ref[2 * tile], out_ref[2 * tile + 1]], axis=1)
        xt = target[:HD].astype(F32)
        zeros = jnp.zeros((HD, 2 * TB), BF16)
        wide_ref[:HALF] = dot(rows_ref[...], jnp.concatenate([target[HD:], zeros], axis=0))
        wide_ref[HALF:] = dot(rows_ref[...], jnp.concatenate([zeros, target[HD:]], axis=0))
        write_features(xt, 2.0, feats_ref)
        values = dot(cols_ref[:HD, :], feats_ref[:HALF]) + dot(cols_ref[HD:, :], feats_ref[HALF:])
        count = HD // GRAIN
        grains = [xt[GRAIN * block : GRAIN * (block + 1)] for block in range(count)]
        sums = [jnp.zeros((GRAIN, 2 * TB), F32) for unused in range(count)]
        for block in range(count):
            rows = []
            for j in range(GRAIN * block, GRAIN * (block + 1)):
                row = xt[j : j + 1]
                across = None
                for other in range(block, count):
                    start = STARTS[j] + GRAIN * (other - block)
                    wide = wide_ref[start : start + GRAIN]
                    sums[other] = sums[other] + row * wide
                    if other > block:
                        term = grains[other] * wide
                        across = term if across is None else across + term
                if across is not None:
                    rows.append(jnp.sum(across, axis=0, keepdims=True))
            if rows:
                sums[block] = sums[block] + jnp.concatenate(rows, axis=0)
        result = local_ref[tile] + jnp.concatenate(
            [
                jnp.concatenate(sums, axis=0) * (2.0 / (HD * HD)),
                values * (1.0 / (HD * HD)),
            ],
            axis=0,
        )
        grads_ref[2 * tile] = result[:, :TB].T
        grads_ref[2 * tile + 1] = result[:, TB:].T
        return carry

    lax.fori_loop(0, BLOCKS // 2, step, 0)


def project_body(grads_ref, wq_ref, wk_ref, wv_ref, out_ref):
    query = jnp.concatenate([grads_ref[2 * h][:, :HD] for h in range(CHIPS)], axis=1)
    key = jnp.concatenate([grads_ref[2 * h + 1][:, :HD] for h in range(CHIPS)], axis=1)
    value = jnp.concatenate([grads_ref[2 * h + 1][:, HD:] for h in range(CHIPS)], axis=1)
    query, key, value = query.astype(BF16), key.astype(BF16), value.astype(BF16)
    width = out_ref.shape[2]
    for place in range(out_ref.shape[0]):
        cols = slice(place * width, (place + 1) * width)
        out_ref[place] = (
            dot(query, wq_ref[:, cols]) + dot(key, wk_ref[:, cols]) + dot(value, wv_ref[:, cols])
        )


def on_device(queries, keys, values, out_grad, w_query, w_key, w_value):
    shape = jax.ShapeDtypeStruct
    groups = lax.axis_size("x") * lax.axis_size("zg")
    packed = call(
        pack_body,
        shape((CHIPS, 2, TB, TB), F32),
        (queries, keys, values, out_grad),
        "pack",
        flops=1 << 20,
        nbytes=1 << 20,
    )
    own = lax.all_to_all(packed, "zc", 0, 0, tiled=True)
    other = lax.ppermute(own, "core", [(0, 1), (1, 0)])
    blocks = shape((BLOCKS, TB, TB), BF16)
    state, tok, src, out = call(
        state_body,
        (shape((HALF, TB), F32), blocks, blocks, blocks),
        (own, other),
        "state",
        scratch=[pltpu.VMEM((PAIRS, 2 * TB), BF16)],
        flops=4 << 30,
        nbytes=3 << 20,
    )
    shards = lax.all_to_all(
        state.reshape(groups, HALF // groups, TB), ("x", "zg"), 0, 0, tiled=True
    )
    local = call(
        local_body,
        shape((BLOCKS // 2, TB, 2 * TB), F32),
        (tok, src, out),
        "local",
        flops=4 << 30,
        nbytes=1 << 20,
    )
    sums = call(
        scan_body, shape(shards.shape, F32), (shards,), "scan", flops=1 << 20, nbytes=1 << 20
    )
    before = lax.all_to_all(sums, ("x", "zg"), 0, 0, tiled=True).reshape(HALF, TB)
    grads = call(
        grads_body,
        shape((BLOCKS, TB, TB), F32),
        (before, out, local),
        "grads",
        scratch=[
            pltpu.VMEM((HALF, TB), BF16),
            pltpu.VMEM((TB, HALF), BF16),
            pltpu.VMEM((PAIRS, 2 * TB), F32),
            pltpu.VMEM((PAIRS, 2 * TB), BF16),
        ],
        flops=4 << 30,
        nbytes=3 << 20,
    )
    mine = lax.all_to_all(grads, ("zc", "core"), 0, 0, tiled=True)
    heads = lax.axis_size("y")
    partial_sum = call(
        project_body,
        shape((heads, TB, w_query.shape[1] // heads), F32),
        (mine, w_query, w_key, w_value),
        "project",
        flops=1 << 29,
        nbytes=4 << 20,
    )
    pieces = lax.all_to_all(partial_sum, "y", 0, 0, tiled=True)
    return jnp.sum(pieces, axis=0).astype(BF16)


def solution(mesh):
    seq, head = mesh.devices.shape
    cols = 4 if seq >= 128 else 2
    grid = Mesh(
        mesh.devices.reshape(seq // (cols * 8), cols, CHIPS, 2, head),
        ("x", "zg", "zc", "core", "y"),
    )
    tokens = ("x", "zg", "zc", "core")
    placed = (P(tokens, "y"),) * 4 + (P("y", None),) * 3
    return jax.shard_map(
        on_device, mesh=grid, in_specs=placed, out_specs=P(tokens, "y"), check_vma=False
    )
```

```python
import functools

import jax
import jax.numpy as jnp
from jax import lax
from jax.experimental import pallas as pl
from jax.experimental.pallas import tpu as pltpu
from jax.sharding import Mesh
from jax.sharding import PartitionSpec as P

HD = 64
TB = 128
CHIPS = 4
BLOCKS = 8
GRAIN = 8
GRAINS = HD // GRAIN
HALF = 1056


def row_tiles():
    off = [
        [("off", j, other) for j in range(GRAIN * block, GRAIN * (block + 1)) for other in range(block + 1, GRAINS)]
        for block in range(GRAINS)
    ]
    ring = [[("ring", block, step) for step in range(GRAIN // 2)] for block in range(GRAINS)]
    left = [("left", block, block + 1) for block in range(0, GRAINS, 2)]
    empty = [("empty", 0, 0)] * 2
    first = off[0] + off[1] + sum(ring[:6], []) + left[:2] + empty
    return first + sum(off[2:], []) + sum(ring[6:], []) + left[2:] + empty


TILES = row_tiles()
assert len(TILES) * GRAIN == 2 * HALF
VMEM = pl.BlockSpec(memory_space=pltpu.VMEM)
F32 = jnp.float32
BF16 = jnp.bfloat16


def call(body, out_shape, args, name, scratch=(), flops=0, nbytes=0):
    return pl.pallas_call(
        body,
        out_shape=out_shape,
        in_specs=[VMEM] * len(args),
        out_specs=jax.tree.map(lambda unused: VMEM, out_shape),
        scratch_shapes=list(scratch),
        name=name,
        compiler_params=pltpu.CompilerParams(vmem_limit_bytes=24 << 20),
        cost_estimate=pl.CostEstimate(flops=flops, bytes_accessed=nbytes, transcendentals=0),
    )(*args)


def dot(a, b):
    return jnp.dot(a, b, preferred_element_type=F32)


def pack_body(q_ref, k_ref, v_ref, g_ref, out_ref):
    for head in range(CHIPS):
        cols = slice(head * HD, (head + 1) * HD)
        out_ref[2 * head] = jnp.concatenate([k_ref[:, cols], v_ref[:, cols]], axis=1).astype(F32)
        out_ref[2 * head + 1] = jnp.concatenate([q_ref[:, cols], g_ref[:, cols]], axis=1).astype(F32)


def turned(grain, step):
    return jnp.concatenate([grain[step:], grain[:step]], axis=0) if step else grain


def write_features(xt, factor, feats_ref):
    grains = [xt[GRAIN * block : GRAIN * (block + 1)] for block in range(GRAINS)]
    twice = [grain * factor for grain in grains] if factor != 1.0 else grains
    half = GRAIN // 2
    tiles = []
    for kind, one, two in TILES:
        if kind == "off":
            tiles.append(xt[one : one + 1] * twice[two])
        elif kind == "ring":
            tiles.append(grains[one] * turned(twice[one] if two else grains[one], two))
        elif kind == "empty":
            tiles.append(jnp.zeros_like(grains[0]))
        else:
            pieces = [grains[block][:half] * twice[block][half:] for block in (one, two)]
            tiles.append(jnp.concatenate(pieces, axis=0))
    for place in range(0, len(tiles), 2):
        rows = slice(GRAIN * place, GRAIN * (place + 2))
        feats_ref[rows, :] = jnp.concatenate(tiles[place : place + 2], axis=0).astype(BF16)


def chain_back(xt, wide_ref):
    grains = [xt[GRAIN * block : GRAIN * (block + 1)] for block in range(GRAINS)]
    sums = [jnp.zeros(grains[0].shape, F32) for unused in range(GRAINS)]
    across = {}
    half = GRAIN // 2
    for place, (kind, one, two) in enumerate(TILES):
        if kind == "empty":
            continue
        wide = wide_ref[GRAIN * place : GRAIN * (place + 1)]
        if kind == "off":
            sums[two] = sums[two] + xt[one : one + 1] * wide
            term = grains[two] * wide
            across[one] = across[one] + term if one in across else term
        elif kind == "ring":
            sums[one] = sums[one] + turned(grains[one], two) * wide
            if two:
                sums[one] = sums[one] + turned(grains[one] * wide, GRAIN - two)
        else:
            for number, block in enumerate((one, two)):
                piece = wide[half * number : half * (number + 1)]
                term = [grains[block][half:] * piece, grains[block][:half] * piece]
                sums[block] = sums[block] + jnp.concatenate(term, axis=0)
    for block in range(GRAINS - 1):
        rows = [
            jnp.sum(across[j], axis=0, keepdims=True)
            for j in range(GRAIN * block, GRAIN * (block + 1))
        ]
        sums[block] = sums[block] + jnp.concatenate(rows, axis=0)
    return jnp.concatenate(sums, axis=0)


def state_body(source_ref, state_ref, tok_ref, src_ref, feats_ref):
    for block in range(BLOCKS):
        source = source_ref[block]
        tok_ref[block] = source.astype(BF16)
        src_ref[block] = source.T.astype(BF16)
    state_ref[...] = jnp.zeros_like(state_ref)

    def step(tile, carry):
        xt = jnp.concatenate([src_ref[2 * tile, :HD], src_ref[2 * tile + 1, :HD]], axis=1)
        write_features(xt.astype(F32), 1.0, feats_ref)
        tok = jnp.concatenate([tok_ref[2 * tile], tok_ref[2 * tile + 1]], axis=0)
        values = tok[:, HD:]
        zeros = jnp.zeros_like(values)
        state_ref[...] += dot(
            feats_ref[:HALF, :], jnp.concatenate([values, zeros], axis=1)
        ) + dot(feats_ref[HALF:, :], jnp.concatenate([zeros, values], axis=1))
        return carry

    lax.fori_loop(0, BLOCKS // 2, step, 0)


def local_body(tok_ref, src_ref, target_ref, local_ref, out_ref):
    core = lax.axis_index("core")
    tiles = BLOCKS // 2
    width = 2 * TB
    sign = 1 - 2 * core
    for block in range(BLOCKS):
        out_ref[block] = target_ref[block].T.astype(BF16)
    local_ref[...] = jnp.zeros_like(local_ref)
    ahead = lax.broadcasted_iota(jnp.int32, (width, width), 0) - lax.broadcasted_iota(
        jnp.int32, (width, width), 1
    )

    def outer(tile, carry):
        target = jnp.concatenate([out_ref[2 * tile], out_ref[2 * tile + 1]], axis=1)
        zeros = jnp.zeros((HD, width), BF16)
        score_rhs = jnp.concatenate([target[:HD], zeros], axis=0)
        value_rhs = jnp.concatenate([zeros, target[HD:]], axis=0)

        def inner(source, carry):
            tok = jnp.concatenate([tok_ref[2 * source], tok_ref[2 * source + 1]], axis=0)
            scores = dot(tok, score_rhs)
            products = dot(tok, value_rhs)
            keep = (ahead + (source - tile) * width) * sign <= 0
            scaled = jnp.where(keep, scores, 0.0) * (1.0 / HD)
            attn = (scaled * scaled).astype(BF16)
            pgrad = (scaled * products * (2.0 / HD)).astype(BF16)
            left = jnp.concatenate([src_ref[2 * source], src_ref[2 * source + 1]], axis=1)
            local_ref[tile, :HD] += dot(left[:HD], pgrad)
            local_ref[tile, HD:] += dot(left[HD:], attn)
            return carry

        first = jnp.where(core == 0, 0, tile)
        last = jnp.where(core == 0, tile + 1, tiles)
        lax.fori_loop(first, last, inner, 0)
        return carry

    lax.fori_loop(0, tiles, outer, 0)


def total_body(parts_ref, total_ref):
    total = parts_ref[0]
    for place in range(1, parts_ref.shape[0]):
        total = total + parts_ref[place]
    for place in range(total_ref.shape[0]):
        total_ref[place] = total


def scan_body(parts_ref, totals_ref, sums_ref):
    core = lax.axis_index("core")
    row = lax.axis_index("x")
    rows = totals_ref.shape[0]
    count = parts_ref.shape[0]

    def add(place, total):
        return total + totals_ref[place]

    first = jnp.where(core == 0, 0, row + 1)
    last = jnp.where(core == 0, row, rows)
    total = lax.fori_loop(first, last, add, jnp.zeros(parts_ref.shape[1:], F32))

    def step(number, total):
        place = number + core * (count - 1 - 2 * number)
        sums_ref[place] = total
        return total + parts_ref[place]

    lax.fori_loop(0, count, step, total)


def grads_body(state_ref, out_ref, local_ref, grads_ref, rows_ref, cols_ref, wide_ref, feats_ref):
    rows_ref[...] = state_ref[...].astype(BF16)
    for start in range(0, HALF, TB):
        stop = min(start + TB, HALF)
        part = state_ref[start:stop, :]
        if stop - start < TB:
            part = jnp.concatenate([part, jnp.zeros((TB - stop + start, TB), F32)], axis=0)
        cols_ref[:, start:stop] = part.T[:, : stop - start].astype(BF16)

    def step(tile, carry):
        target = jnp.concatenate([out_ref[2 * tile], out_ref[2 * tile + 1]], axis=1)
        xt = target[:HD].astype(F32)
        zeros = jnp.zeros((HD, 2 * TB), BF16)
        wide_ref[:HALF] = dot(rows_ref[...], jnp.concatenate([target[HD:], zeros], axis=0))
        wide_ref[HALF:] = dot(rows_ref[...], jnp.concatenate([zeros, target[HD:]], axis=0))
        write_features(xt, 2.0, feats_ref)
        values = dot(cols_ref[:HD, :], feats_ref[:HALF]) + dot(cols_ref[HD:, :], feats_ref[HALF:])
        result = local_ref[tile] + jnp.concatenate(
            [chain_back(xt, wide_ref) * (2.0 / (HD * HD)), values * (1.0 / (HD * HD))], axis=0
        )
        grads_ref[2 * tile] = result[:, :TB].T
        grads_ref[2 * tile + 1] = result[:, TB:].T
        return carry

    lax.fori_loop(0, BLOCKS // 2, step, 0)


def project_body(grads_ref, wq_ref, wk_ref, wv_ref, out_ref):
    query = jnp.concatenate([grads_ref[2 * h][:, :HD] for h in range(CHIPS)], axis=1)
    key = jnp.concatenate([grads_ref[2 * h + 1][:, :HD] for h in range(CHIPS)], axis=1)
    value = jnp.concatenate([grads_ref[2 * h + 1][:, HD:] for h in range(CHIPS)], axis=1)
    query, key, value = query.astype(BF16), key.astype(BF16), value.astype(BF16)
    width = out_ref.shape[2]
    for place in range(out_ref.shape[0]):
        cols = slice(place * width, (place + 1) * width)
        out_ref[place] = (
            dot(query, wq_ref[:, cols]) + dot(key, wk_ref[:, cols]) + dot(value, wv_ref[:, cols])
        )


def on_device(queries, keys, values, out_grad, w_query, w_key, w_value):
    shape = jax.ShapeDtypeStruct
    rows, cols = lax.axis_size("x"), lax.axis_size("zg")
    packed = call(
        pack_body,
        shape((BLOCKS, TB, TB), F32),
        (queries, keys, values, out_grad),
        "pack",
        flops=1 << 20,
        nbytes=1 << 20,
    )
    source = lax.all_to_all(packed, ("zc", "core"), 0, 0, tiled=True)
    target = lax.ppermute(source, "core", [(0, 1), (1, 0)])
    blocks = shape((BLOCKS, TB, TB), BF16)
    state, tok, src = call(
        state_body,
        (shape((HALF, TB), F32), blocks, blocks),
        (source,),
        "state",
        scratch=[pltpu.VMEM((2 * HALF, 2 * TB), BF16)],
        flops=4 << 30,
        nbytes=3 << 20,
    )
    parts = lax.all_to_all(state.reshape(cols, HALF // cols, TB), "zg", 0, 0, tiled=True)
    total = call(
        total_body,
        shape((rows, HALF // cols, TB), F32),
        (parts,),
        "total",
        flops=1 << 20,
        nbytes=1 << 20,
    )
    totals = lax.all_to_all(total, "x", 0, 0, tiled=True)
    sums = call(
        scan_body,
        shape(parts.shape, F32),
        (parts, totals),
        "scan",
        flops=1 << 20,
        nbytes=1 << 20,
    )
    before = lax.all_to_all(sums, "zg", 0, 0, tiled=True).reshape(HALF, TB)
    local, out = call(
        local_body,
        (shape((BLOCKS // 2, TB, 2 * TB), F32), blocks),
        (tok, src, target),
        "local",
        flops=4 << 30,
        nbytes=1 << 20,
    )
    grads = call(
        grads_body,
        shape((BLOCKS, TB, TB), F32),
        (before, out, local),
        "grads",
        scratch=[
            pltpu.VMEM((HALF, TB), BF16),
            pltpu.VMEM((TB, HALF), BF16),
            pltpu.VMEM((2 * HALF, 2 * TB), F32),
            pltpu.VMEM((2 * HALF, 2 * TB), BF16),
        ],
        flops=4 << 30,
        nbytes=3 << 20,
    )
    mine = lax.all_to_all(grads, ("zc", "core"), 0, 0, tiled=True)
    heads = lax.axis_size("y")
    partial_sum = call(
        project_body,
        shape((heads, TB, w_query.shape[1] // heads), F32),
        (mine, w_query, w_key, w_value),
        "project",
        flops=1 << 29,
        nbytes=4 << 20,
    )
    pieces = lax.all_to_all(partial_sum, "y", 0, 0, tiled=True)
    return jnp.sum(pieces, axis=0).astype(BF16)


def solution(mesh):
    seq, head = mesh.devices.shape
    cols = 4 if seq >= 128 else 2
    grid = Mesh(
        mesh.devices.reshape(seq // (cols * 8), cols, CHIPS, 2, head),
        ("x", "zg", "zc", "core", "y"),
    )
    tokens = ("x", "zg", "zc", "core")
    placed = (P(tokens, "y"),) * 4 + (P("y", None),) * 3
    return jax.shard_map(
        on_device, mesh=grid, in_specs=placed, out_specs=P(tokens, "y"), check_vma=False
    )
```

```python
import functools

import jax
import jax.numpy as jnp
from jax import lax
from jax.experimental import pallas as pl
from jax.experimental.pallas import tpu as pltpu
from jax.sharding import Mesh
from jax.sharding import PartitionSpec as P

HD = 64
TB = 128
CHIPS = 4
BLOCKS = 8
GRAIN = 8
GRAINS = HD // GRAIN
HALF = 1040


def row_tiles():
    off = [
        [("off", j, other) for j in range(GRAIN * block, GRAIN * (block + 1)) for other in range(block + 1, GRAINS)]
        for block in range(GRAINS)
    ]
    ring = [[("ring", block, step) for step in range(GRAIN // 2)] for block in range(GRAINS)]
    left = [("left", block, block + 1) for block in range(0, GRAINS, 2)]
    first = off[0] + off[1] + sum(ring[:6], []) + left[:2]
    return first + sum(off[2:], []) + sum(ring[6:], []) + left[2:]


TILES = row_tiles()
assert len(TILES) * GRAIN == 2 * HALF
VMEM = pl.BlockSpec(memory_space=pltpu.VMEM)
F32 = jnp.float32
BF16 = jnp.bfloat16


def call(body, out_shape, args, name, scratch=(), flops=0, nbytes=0, limit=24 << 20):
    return pl.pallas_call(
        body,
        out_shape=out_shape,
        in_specs=[VMEM] * len(args),
        out_specs=jax.tree.map(lambda unused: VMEM, out_shape),
        scratch_shapes=list(scratch),
        name=name,
        compiler_params=pltpu.CompilerParams(vmem_limit_bytes=limit),
        cost_estimate=pl.CostEstimate(flops=flops, bytes_accessed=nbytes, transcendentals=0),
    )(*args)


def dot(a, b):
    return jnp.dot(a, b, preferred_element_type=F32)


def pack_body(q_ref, k_ref, v_ref, g_ref, out_ref):
    for head in range(CHIPS):
        cols = slice(head * HD, (head + 1) * HD)
        out_ref[2 * head] = jnp.concatenate([k_ref[:, cols], v_ref[:, cols]], axis=1).astype(F32)
        out_ref[2 * head + 1] = jnp.concatenate([q_ref[:, cols], g_ref[:, cols]], axis=1).astype(F32)


def turned(grain, step):
    return jnp.concatenate([grain[step:], grain[:step]], axis=0) if step else grain


def write_features(xt, factor, feats_ref):
    grains = [xt[GRAIN * block : GRAIN * (block + 1)] for block in range(GRAINS)]
    twice = [grain * factor for grain in grains] if factor != 1.0 else grains
    half = GRAIN // 2
    tiles = []
    for kind, one, two in TILES:
        if kind == "off":
            tiles.append(xt[one : one + 1] * twice[two])
        elif kind == "ring":
            tiles.append(grains[one] * turned(twice[one] if two else grains[one], two))
        else:
            pieces = [grains[block][:half] * twice[block][half:] for block in (one, two)]
            tiles.append(jnp.concatenate(pieces, axis=0))
    for place in range(0, len(tiles), 2):
        rows = slice(GRAIN * place, GRAIN * (place + 2))
        feats_ref[rows, :] = jnp.concatenate(tiles[place : place + 2], axis=0).astype(BF16)


def chain_back(xt, wide_ref):
    grains = [xt[GRAIN * block : GRAIN * (block + 1)] for block in range(GRAINS)]
    sums = [jnp.zeros(grains[0].shape, F32) for unused in range(GRAINS)]
    across = {}
    half = GRAIN // 2
    for place, (kind, one, two) in enumerate(TILES):
        wide = wide_ref[GRAIN * place : GRAIN * (place + 1)]
        if kind == "off":
            sums[two] = sums[two] + xt[one : one + 1] * wide
            term = grains[two] * wide
            across[one] = across[one] + term if one in across else term
        elif kind == "ring":
            sums[one] = sums[one] + turned(grains[one], two) * wide
            if two:
                sums[one] = sums[one] + turned(grains[one] * wide, GRAIN - two)
        else:
            for number, block in enumerate((one, two)):
                piece = wide[half * number : half * (number + 1)]
                term = [grains[block][half:] * piece, grains[block][:half] * piece]
                sums[block] = sums[block] + jnp.concatenate(term, axis=0)
    for block in range(GRAINS - 1):
        rows = [
            jnp.sum(across[j], axis=0, keepdims=True)
            for j in range(GRAIN * block, GRAIN * (block + 1))
        ]
        sums[block] = sums[block] + jnp.concatenate(rows, axis=0)
    return jnp.concatenate(sums, axis=0)


def state_body(source_ref, state_ref, tok_ref, src_ref, feats_ref):
    for block in range(BLOCKS):
        source = source_ref[block]
        tok_ref[block] = source.astype(BF16)
        src_ref[block] = source.T.astype(BF16)
    state_ref[...] = jnp.zeros_like(state_ref)

    def step(tile, carry):
        xt = jnp.concatenate([src_ref[2 * tile, :HD], src_ref[2 * tile + 1, :HD]], axis=1)
        write_features(xt.astype(F32), 1.0, feats_ref)
        tok = jnp.concatenate([tok_ref[2 * tile], tok_ref[2 * tile + 1]], axis=0)
        values = tok[:, HD:]
        zeros = jnp.zeros_like(values)
        state_ref[...] += dot(
            feats_ref[:HALF, :], jnp.concatenate([values, zeros], axis=1)
        ) + dot(feats_ref[HALF:, :], jnp.concatenate([zeros, values], axis=1))
        return carry

    lax.fori_loop(0, BLOCKS // 2, step, 0)


def local_body(tok_ref, src_ref, target_ref, local_ref, out_ref):
    core = lax.axis_index("core")
    tiles = BLOCKS // 2
    width = 2 * TB
    sign = 1 - 2 * core
    for block in range(BLOCKS):
        out_ref[block] = target_ref[block].T.astype(BF16)
    local_ref[...] = jnp.zeros_like(local_ref)
    ahead = lax.broadcasted_iota(jnp.int32, (width, width), 0) - lax.broadcasted_iota(
        jnp.int32, (width, width), 1
    )

    def outer(tile, carry):
        target = jnp.concatenate([out_ref[2 * tile], out_ref[2 * tile + 1]], axis=1)
        zeros = jnp.zeros((HD, width), BF16)
        score_rhs = jnp.concatenate([target[:HD], zeros], axis=0)
        value_rhs = jnp.concatenate([zeros, target[HD:]], axis=0)

        def inner(source, carry):
            tok = jnp.concatenate([tok_ref[2 * source], tok_ref[2 * source + 1]], axis=0)
            scores = dot(tok, score_rhs)
            products = dot(tok, value_rhs)
            keep = (ahead + (source - tile) * width) * sign <= 0
            scaled = jnp.where(keep, scores, 0.0) * (1.0 / HD)
            attn = (scaled * scaled).astype(BF16)
            pgrad = (scaled * products * (2.0 / HD)).astype(BF16)
            left = jnp.concatenate([src_ref[2 * source], src_ref[2 * source + 1]], axis=1)
            local_ref[tile, :HD] += dot(left[:HD], pgrad)
            local_ref[tile, HD:] += dot(left[HD:], attn)
            return carry

        first = jnp.where(core == 0, 0, tile)
        last = jnp.where(core == 0, tile + 1, tiles)
        lax.fori_loop(first, last, inner, 0)
        return carry

    lax.fori_loop(0, tiles, outer, 0)


def scan_body(parts_ref, sums_ref):
    core = lax.axis_index("core")
    count = parts_ref.shape[0]

    def step(number, total):
        place = number + core * (count - 1 - 2 * number)
        sums_ref[place] = total
        return total + parts_ref[place]

    lax.fori_loop(0, count, step, jnp.zeros(parts_ref.shape[1:], F32))


def grads_body(state_ref, out_ref, local_ref, grads_ref, rows_ref, cols_ref, wide_ref, feats_ref):
    keyed = lax.axis_index("core") == 1
    rows_ref[...] = state_ref[...].astype(BF16)

    @pl.when(keyed)
    def turn():
        for start in range(0, HALF, TB):
            stop = min(start + TB, HALF)
            part = state_ref[start:stop, :]
            if stop - start < TB:
                part = jnp.concatenate([part, jnp.zeros((TB - stop + start, TB), F32)], axis=0)
            cols_ref[:, start:stop] = part.T[:, : stop - start].astype(BF16)

    def step(tile, carry):
        target = jnp.concatenate([out_ref[2 * tile], out_ref[2 * tile + 1]], axis=1)
        xt = target[:HD].astype(F32)
        zeros = jnp.zeros((HD, 2 * TB), BF16)
        wide_ref[:HALF] = dot(rows_ref[...], jnp.concatenate([target[HD:], zeros], axis=0))
        wide_ref[HALF:] = dot(rows_ref[...], jnp.concatenate([zeros, target[HD:]], axis=0))
        result = local_ref[tile, :HD] + chain_back(xt, wide_ref) * (2.0 / (HD * HD))
        grads_ref[2 * tile, :, :HD] = result[:, :TB].T
        grads_ref[2 * tile + 1, :, :HD] = result[:, TB:].T

        @pl.when(keyed)
        def value_part():
            write_features(xt, 2.0, feats_ref)
            values = dot(cols_ref[:HD, :], feats_ref[:HALF]) + dot(
                cols_ref[HD:, :], feats_ref[HALF:]
            )
            total = local_ref[tile, HD:] + values * (1.0 / (HD * HD))
            grads_ref[2 * tile, :, HD:] = total[:, :TB].T
            grads_ref[2 * tile + 1, :, HD:] = total[:, TB:].T

        @pl.when(jnp.logical_not(keyed))
        def no_values():
            grads_ref[2 * tile, :, HD:] = jnp.zeros((TB, HD), F32)
            grads_ref[2 * tile + 1, :, HD:] = jnp.zeros((TB, HD), F32)

        return carry

    lax.fori_loop(0, BLOCKS // 2, step, 0)


def project_body(grads_ref, wq_ref, wk_ref, wv_ref, out_ref):
    query = jnp.concatenate([grads_ref[2 * h][:, :HD] for h in range(CHIPS)], axis=1)
    key = jnp.concatenate([grads_ref[2 * h + 1][:, :HD] for h in range(CHIPS)], axis=1)
    value = jnp.concatenate([grads_ref[2 * h + 1][:, HD:] for h in range(CHIPS)], axis=1)
    query, key, value = query.astype(BF16), key.astype(BF16), value.astype(BF16)
    width = out_ref.shape[2]
    for place in range(out_ref.shape[0]):
        cols = slice(place * width, (place + 1) * width)
        out_ref[place] = (
            dot(query, wq_ref[:, cols]) + dot(key, wk_ref[:, cols]) + dot(value, wv_ref[:, cols])
        )


def on_device(queries, keys, values, out_grad, w_query, w_key, w_value):
    shape = jax.ShapeDtypeStruct
    groups = lax.axis_size("x") * lax.axis_size("zg")
    packed = call(
        pack_body,
        shape((BLOCKS, TB, TB), F32),
        (queries, keys, values, out_grad),
        "pack",
        limit=None,
        flops=1 << 20,
        nbytes=1 << 20,
    )
    source = lax.all_to_all(packed, ("zc", "core"), 0, 0, tiled=True)
    target = lax.ppermute(source, "core", [(0, 1), (1, 0)])
    blocks = shape((BLOCKS, TB, TB), BF16)
    state, tok, src = call(
        state_body,
        (shape((HALF, TB), F32), blocks, blocks),
        (source,),
        "state",
        scratch=[pltpu.VMEM((2 * HALF, 2 * TB), BF16)],
        flops=4 << 30,
        nbytes=3 << 20,
    )
    parts = lax.all_to_all(
        state.reshape(groups, 1, HALF * TB // groups), ("x", "zg"), 0, 0, tiled=True
    )
    sums = call(
        scan_body, shape(parts.shape, F32), (parts,), "scan", flops=1 << 20, nbytes=1 << 20
    )
    before = lax.all_to_all(sums, ("x", "zg"), 0, 0, tiled=True).reshape(HALF, TB)
    local, out = call(
        local_body,
        (shape((BLOCKS // 2, TB, 2 * TB), F32), blocks),
        (tok, src, target),
        "local",
        flops=4 << 30,
        nbytes=1 << 20,
    )
    grads = call(
        grads_body,
        shape((BLOCKS, TB, TB), F32),
        (before, out, local),
        "grads",
        scratch=[
            pltpu.VMEM((HALF, TB), BF16),
            pltpu.VMEM((TB, HALF), BF16),
            pltpu.VMEM((2 * HALF, 2 * TB), F32),
            pltpu.VMEM((2 * HALF, 2 * TB), BF16),
        ],
        flops=4 << 30,
        nbytes=3 << 20,
    )
    mine = lax.all_to_all(grads, ("zc", "core"), 0, 0, tiled=True)
    heads = lax.axis_size("y")
    partial_sum = call(
        project_body,
        shape((heads, TB, w_query.shape[1] // heads), F32),
        (mine, w_query, w_key, w_value),
        "project",
        flops=1 << 29,
        nbytes=4 << 20,
    )
    pieces = lax.all_to_all(partial_sum, "y", 0, 0, tiled=True)
    return jnp.sum(pieces, axis=0).astype(BF16)


def solution(mesh):
    seq, head = mesh.devices.shape
    cols = 4 if seq >= 128 else 2
    grid = Mesh(
        mesh.devices.reshape(seq // (cols * 8), cols, CHIPS, 2, head),
        ("x", "zg", "zc", "core", "y"),
    )
    tokens = ("x", "zg", "zc", "core")
    placed = (P(tokens, "y"),) * 4 + (P("y", None),) * 3
    return jax.shard_map(
        on_device, mesh=grid, in_specs=placed, out_specs=P(tokens, "y"), check_vma=False
    )
```

```python
import functools

import jax
import jax.numpy as jnp
from jax import lax
from jax.experimental import pallas as pl
from jax.experimental.pallas import tpu as pltpu
from jax.sharding import Mesh
from jax.sharding import PartitionSpec as P

HD = 64
TB = 128
CHIPS = 4
BLOCKS = 8
GRAIN = 8
GRAINS = HD // GRAIN
HALF = 1040


def row_tiles():
    off = [
        [("off", j, other) for j in range(GRAIN * block, GRAIN * (block + 1)) for other in range(block + 1, GRAINS)]
        for block in range(GRAINS)
    ]
    ring = [[("ring", block, step) for step in range(GRAIN // 2)] for block in range(GRAINS)]
    left = [("left", block, block + 1) for block in range(0, GRAINS, 2)]
    first = off[0] + off[1] + sum(ring[:6], []) + left[:2]
    return first + sum(off[2:], []) + sum(ring[6:], []) + left[2:]


TILES = row_tiles()
assert len(TILES) * GRAIN == 2 * HALF
VMEM = pl.BlockSpec(memory_space=pltpu.VMEM)
F32 = jnp.float32
BF16 = jnp.bfloat16


def call(body, out_shape, args, name, scratch=(), flops=0, nbytes=0, limit=24 << 20):
    return pl.pallas_call(
        body,
        out_shape=out_shape,
        in_specs=[VMEM] * len(args),
        out_specs=jax.tree.map(lambda unused: VMEM, out_shape),
        scratch_shapes=list(scratch),
        name=name,
        compiler_params=pltpu.CompilerParams(vmem_limit_bytes=limit),
        cost_estimate=pl.CostEstimate(flops=flops, bytes_accessed=nbytes, transcendentals=0),
    )(*args)


def dot(a, b):
    return jnp.dot(a, b, preferred_element_type=F32)


def pack_body(q_ref, k_ref, v_ref, g_ref, out_ref):
    for head in range(CHIPS):
        cols = slice(head * HD, (head + 1) * HD)
        out_ref[2 * head] = jnp.concatenate([k_ref[:, cols], v_ref[:, cols]], axis=1).astype(F32)
        out_ref[2 * head + 1] = jnp.concatenate([q_ref[:, cols], g_ref[:, cols]], axis=1).astype(F32)


def turned(grain, step):
    return jnp.concatenate([grain[step:], grain[:step]], axis=0) if step else grain


def write_features(xt, factor, feats_ref):
    grains = [xt[GRAIN * block : GRAIN * (block + 1)] for block in range(GRAINS)]
    twice = [grain * factor for grain in grains] if factor != 1.0 else grains
    half = GRAIN // 2
    tiles = []
    for kind, one, two in TILES:
        if kind == "off":
            tiles.append(xt[one : one + 1] * twice[two])
        elif kind == "ring":
            tiles.append(grains[one] * turned(twice[one] if two else grains[one], two))
        else:
            pieces = [grains[block][:half] * twice[block][half:] for block in (one, two)]
            tiles.append(jnp.concatenate(pieces, axis=0))
    for place in range(0, len(tiles), 2):
        rows = slice(GRAIN * place, GRAIN * (place + 2))
        feats_ref[rows, :] = jnp.concatenate(tiles[place : place + 2], axis=0).astype(BF16)


def chain_back(xt, wide_ref):
    grains = [xt[GRAIN * block : GRAIN * (block + 1)] for block in range(GRAINS)]
    sums = [jnp.zeros(grains[0].shape, F32) for unused in range(GRAINS)]
    across = {}
    half = GRAIN // 2
    for place, (kind, one, two) in enumerate(TILES):
        wide = wide_ref[GRAIN * place : GRAIN * (place + 1)]
        if kind == "off":
            sums[two] = sums[two] + xt[one : one + 1] * wide
            term = grains[two] * wide
            across[one] = across[one] + term if one in across else term
        elif kind == "ring":
            sums[one] = sums[one] + turned(grains[one], two) * wide
            if two:
                sums[one] = sums[one] + turned(grains[one] * wide, GRAIN - two)
        else:
            for number, block in enumerate((one, two)):
                piece = wide[half * number : half * (number + 1)]
                term = [grains[block][half:] * piece, grains[block][:half] * piece]
                sums[block] = sums[block] + jnp.concatenate(term, axis=0)
    for block in range(GRAINS - 1):
        rows = [
            jnp.sum(across[j], axis=0, keepdims=True)
            for j in range(GRAIN * block, GRAIN * (block + 1))
        ]
        sums[block] = sums[block] + jnp.concatenate(rows, axis=0)
    return jnp.concatenate(sums, axis=0)


def state_body(source_ref, unused_ref, state_ref, tok_ref, src_ref, feats_ref):
    for block in range(BLOCKS):
        source = source_ref[block]
        tok_ref[block] = source.astype(BF16)
        src_ref[block] = source.T.astype(BF16)
    state_ref[...] = jnp.zeros_like(state_ref)

    def step(tile, carry):
        xt = jnp.concatenate([src_ref[2 * tile, :HD], src_ref[2 * tile + 1, :HD]], axis=1)
        write_features(xt.astype(F32), 1.0, feats_ref)
        tok = jnp.concatenate([tok_ref[2 * tile], tok_ref[2 * tile + 1]], axis=0)
        values = tok[:, HD:]
        zeros = jnp.zeros_like(values)
        state_ref[...] += dot(
            feats_ref[:HALF, :], jnp.concatenate([values, zeros], axis=1)
        ) + dot(feats_ref[HALF:, :], jnp.concatenate([zeros, values], axis=1))
        return carry

    lax.fori_loop(0, BLOCKS // 2, step, 0)


def tick_body(unused_ref, tick_ref):
    tick_ref[...] = jnp.zeros_like(tick_ref)


def local_body(tiles, first_tile, tok_ref, src_ref, target_ref, local_ref, *out_refs):
    core = lax.axis_index("core")
    width = 2 * TB
    sign = 1 - 2 * core
    out_ref = target_ref
    if out_refs:
        out_ref = out_refs[0]
        for block in range(BLOCKS):
            out_ref[block] = target_ref[block].T.astype(BF16)
    local_ref[...] = jnp.zeros_like(local_ref)
    ahead = lax.broadcasted_iota(jnp.int32, (width, width), 0) - lax.broadcasted_iota(
        jnp.int32, (width, width), 1
    )

    def outer(number, carry):
        tile = first_tile + number
        target = jnp.concatenate([out_ref[2 * tile], out_ref[2 * tile + 1]], axis=1)
        zeros = jnp.zeros((HD, width), BF16)
        score_rhs = jnp.concatenate([target[:HD], zeros], axis=0)
        value_rhs = jnp.concatenate([zeros, target[HD:]], axis=0)

        def inner(source, carry):
            tok = jnp.concatenate([tok_ref[2 * source], tok_ref[2 * source + 1]], axis=0)
            scores = dot(tok, score_rhs)
            products = dot(tok, value_rhs)
            keep = (ahead + (source - tile) * width) * sign <= 0
            scaled = jnp.where(keep, scores, 0.0) * (1.0 / HD)
            attn = (scaled * scaled).astype(BF16)
            pgrad = (scaled * products * (2.0 / HD)).astype(BF16)
            left = jnp.concatenate([src_ref[2 * source], src_ref[2 * source + 1]], axis=1)
            local_ref[number, :HD] += dot(left[:HD], pgrad)
            local_ref[number, HD:] += dot(left[HD:], attn)
            return carry

        first = jnp.where(core == 0, 0, tile)
        last = jnp.where(core == 0, tile + 1, BLOCKS // 2)
        lax.fori_loop(first, last, inner, 0)
        return carry

    lax.fori_loop(0, tiles, outer, 0)


def scan_body(parts_ref, unused_ref, sums_ref):
    core = lax.axis_index("core")
    count = parts_ref.shape[0]

    def step(number, total):
        place = number + core * (count - 1 - 2 * number)
        sums_ref[place] = total
        return total + parts_ref[place]

    lax.fori_loop(0, count, step, jnp.zeros(parts_ref.shape[1:], F32))


def grads_body(state_ref, out_ref, early_ref, late_ref, grads_ref, rows_ref, cols_ref, wide_ref, feats_ref):
    rows_ref[...] = state_ref[...].astype(BF16)
    for start in range(0, HALF, TB):
        stop = min(start + TB, HALF)
        part = state_ref[start:stop, :]
        if stop - start < TB:
            part = jnp.concatenate([part, jnp.zeros((TB - stop + start, TB), F32)], axis=0)
        cols_ref[:, start:stop] = part.T[:, : stop - start].astype(BF16)

    def step(tile, carry):
        target = jnp.concatenate([out_ref[2 * tile], out_ref[2 * tile + 1]], axis=1)
        xt = target[:HD].astype(F32)
        zeros = jnp.zeros((HD, 2 * TB), BF16)
        wide_ref[:HALF] = dot(rows_ref[...], jnp.concatenate([target[HD:], zeros], axis=0))
        wide_ref[HALF:] = dot(rows_ref[...], jnp.concatenate([zeros, target[HD:]], axis=0))
        write_features(xt, 2.0, feats_ref)
        values = dot(cols_ref[:HD, :], feats_ref[:HALF]) + dot(cols_ref[HD:, :], feats_ref[HALF:])
        local = jnp.where(tile < 2, early_ref[tile % 2], late_ref[tile % 2])
        result = local + jnp.concatenate(
            [chain_back(xt, wide_ref) * (2.0 / (HD * HD)), values * (1.0 / (HD * HD))], axis=0
        )
        grads_ref[2 * tile] = result[:, :TB].T
        grads_ref[2 * tile + 1] = result[:, TB:].T
        return carry

    lax.fori_loop(0, BLOCKS // 2, step, 0)


def project_body(grads_ref, unused_ref, wq_ref, wk_ref, wv_ref, out_ref):
    query = jnp.concatenate([grads_ref[2 * h][:, :HD] for h in range(CHIPS)], axis=1)
    key = jnp.concatenate([grads_ref[2 * h + 1][:, :HD] for h in range(CHIPS)], axis=1)
    value = jnp.concatenate([grads_ref[2 * h + 1][:, HD:] for h in range(CHIPS)], axis=1)
    query, key, value = query.astype(BF16), key.astype(BF16), value.astype(BF16)
    width = out_ref.shape[2]
    for place in range(out_ref.shape[0]):
        cols = slice(place * width, (place + 1) * width)
        out_ref[place] = (
            dot(query, wq_ref[:, cols]) + dot(key, wk_ref[:, cols]) + dot(value, wv_ref[:, cols])
        )


def finish_body(pieces_ref, unused_ref, out_ref):
    total = pieces_ref[0]
    for place in range(1, pieces_ref.shape[0]):
        total = total + pieces_ref[place]
    out_ref[...] = total.astype(BF16)


def on_device(queries, keys, values, out_grad, w_query, w_key, w_value):
    shape = jax.ShapeDtypeStruct
    groups = lax.axis_size("x") * lax.axis_size("zg")
    packed = call(
        pack_body,
        shape((BLOCKS, TB, TB), F32),
        (queries, keys, values, out_grad),
        "pack",
        limit=None,
        flops=1 << 20,
        nbytes=1 << 20,
    )
    def tick(value, name):
        return call(tick_body, shape((8, TB), F32), (value,), name, flops=1 << 20, nbytes=1 << 12)

    source = lax.all_to_all(packed, ("zc", "core"), 0, 0, tiled=True)
    target = lax.ppermute(source, "core", [(0, 1), (1, 0)])
    blocks = shape((BLOCKS, TB, TB), BF16)
    state, tok, src = call(
        state_body,
        (shape((HALF, TB), F32), blocks, blocks),
        (source, tick(packed, "tick_in")),
        "state",
        scratch=[pltpu.VMEM((2 * HALF, 2 * TB), BF16)],
        flops=4 << 30,
        nbytes=3 << 20,
    )
    parts = lax.all_to_all(
        state.reshape(groups, 1, HALF * TB // groups), ("x", "zg"), 0, 0, tiled=True
    )
    tiles = BLOCKS // 4
    halves = shape((tiles, TB, 2 * TB), F32)
    early, out = call(
        functools.partial(local_body, tiles, 0),
        (halves, blocks),
        (tok, src, target),
        "early",
        flops=2 << 30,
        nbytes=1 << 20,
    )
    sums = call(
        scan_body, shape(parts.shape, F32), (parts, early), "scan", flops=1 << 20, nbytes=1 << 20
    )
    before = lax.all_to_all(sums, ("x", "zg"), 0, 0, tiled=True).reshape(HALF, TB)
    (late,) = call(
        functools.partial(local_body, tiles, tiles),
        (halves,),
        (tok, src, out),
        "late",
        flops=2 << 30,
        nbytes=1 << 20,
    )
    grads = call(
        grads_body,
        shape((BLOCKS, TB, TB), F32),
        (before, out, early, late),
        "grads",
        scratch=[
            pltpu.VMEM((HALF, TB), BF16),
            pltpu.VMEM((TB, HALF), BF16),
            pltpu.VMEM((2 * HALF, 2 * TB), F32),
            pltpu.VMEM((2 * HALF, 2 * TB), BF16),
        ],
        flops=4 << 30,
        nbytes=3 << 20,
    )
    mine = lax.all_to_all(grads, ("zc", "core"), 0, 0, tiled=True)
    heads = lax.axis_size("y")
    partial_sum = call(
        project_body,
        shape((heads, TB, w_query.shape[1] // heads), F32),
        (mine, tick(grads, "tick_grads"), w_query, w_key, w_value),
        "project",
        flops=1 << 29,
        nbytes=4 << 20,
    )
    pieces = lax.all_to_all(partial_sum, "y", 0, 0, tiled=True)
    return call(
        finish_body,
        shape(pieces.shape[1:], BF16),
        (pieces, tick(partial_sum, "tick_out")),
        "finish",
        flops=1 << 20,
        nbytes=1 << 20,
    )


def solution(mesh):
    seq, head = mesh.devices.shape
    cols = 4 if seq >= 128 else 2
    grid = Mesh(
        mesh.devices.reshape(seq // (cols * 8), cols, CHIPS, 2, head),
        ("x", "zg", "zc", "core", "y"),
    )
    tokens = ("x", "zg", "zc", "core")
    placed = (P(tokens, "y"),) * 4 + (P("y", None),) * 3
    return jax.shard_map(
        on_device, mesh=grid, in_specs=placed, out_specs=P(tokens, "y"), check_vma=False
    )
```

```python
import functools

import jax
import jax.numpy as jnp
from jax import lax
from jax.experimental import pallas as pl
from jax.experimental.pallas import tpu as pltpu
from jax.sharding import Mesh
from jax.sharding import PartitionSpec as P

HD = 64
TB = 128
CHIPS = 4
BLOCKS = 8
GRAIN = 8
GRAINS = HD // GRAIN
HALF = 1040


def row_tiles():
    off = [
        [("off", j, other) for j in range(GRAIN * block, GRAIN * (block + 1)) for other in range(block + 1, GRAINS)]
        for block in range(GRAINS)
    ]
    ring = [[("ring", block, step) for step in range(GRAIN // 2)] for block in range(GRAINS)]
    left = [("left", block, block + 1) for block in range(0, GRAINS, 2)]
    first = off[0] + off[1] + sum(ring[:6], []) + left[:2]
    return first + sum(off[2:], []) + sum(ring[6:], []) + left[2:]


TILES = row_tiles()
assert len(TILES) * GRAIN == 2 * HALF
VMEM = pl.BlockSpec(memory_space=pltpu.VMEM)
F32 = jnp.float32
BF16 = jnp.bfloat16


def call(body, out_shape, args, name, scratch=(), flops=0, nbytes=0, limit=24 << 20):
    return pl.pallas_call(
        body,
        out_shape=out_shape,
        in_specs=[VMEM] * len(args),
        out_specs=jax.tree.map(lambda unused: VMEM, out_shape),
        scratch_shapes=list(scratch),
        name=name,
        compiler_params=pltpu.CompilerParams(vmem_limit_bytes=limit),
        cost_estimate=pl.CostEstimate(flops=flops, bytes_accessed=nbytes, transcendentals=0),
    )(*args)


def dot(a, b):
    return jnp.dot(a, b, preferred_element_type=F32)


def pack_body(q_ref, k_ref, v_ref, g_ref, out_ref):
    for head in range(CHIPS):
        cols = slice(head * HD, (head + 1) * HD)
        out_ref[2 * head] = jnp.concatenate([k_ref[:, cols], v_ref[:, cols]], axis=1).astype(F32)
        out_ref[2 * head + 1] = jnp.concatenate([q_ref[:, cols], g_ref[:, cols]], axis=1).astype(F32)


def turned(grain, step):
    return jnp.concatenate([grain[step:], grain[:step]], axis=0) if step else grain


def write_features(xt, factor, feats_ref):
    grains = [xt[GRAIN * block : GRAIN * (block + 1)] for block in range(GRAINS)]
    twice = [grain * factor for grain in grains] if factor != 1.0 else grains
    half = GRAIN // 2
    tiles = []
    for kind, one, two in TILES:
        if kind == "off":
            tiles.append(xt[one : one + 1] * twice[two])
        elif kind == "ring":
            tiles.append(grains[one] * turned(twice[one] if two else grains[one], two))
        else:
            pieces = [grains[block][:half] * twice[block][half:] for block in (one, two)]
            tiles.append(jnp.concatenate(pieces, axis=0))
    for place in range(0, len(tiles), 2):
        rows = slice(GRAIN * place, GRAIN * (place + 2))
        feats_ref[rows, :] = jnp.concatenate(tiles[place : place + 2], axis=0).astype(BF16)


def chain_back(xt, wide_ref):
    grains = [xt[GRAIN * block : GRAIN * (block + 1)] for block in range(GRAINS)]
    sums = [jnp.zeros(grains[0].shape, F32) for unused in range(GRAINS)]
    across = {}
    half = GRAIN // 2
    for place, (kind, one, two) in enumerate(TILES):
        wide = wide_ref[GRAIN * place : GRAIN * (place + 1)]
        if kind == "off":
            sums[two] = sums[two] + xt[one : one + 1] * wide
            term = grains[two] * wide
            across[one] = across[one] + term if one in across else term
        elif kind == "ring":
            sums[one] = sums[one] + turned(grains[one], two) * wide
            if two:
                sums[one] = sums[one] + turned(grains[one] * wide, GRAIN - two)
        else:
            for number, block in enumerate((one, two)):
                piece = wide[half * number : half * (number + 1)]
                term = [grains[block][half:] * piece, grains[block][:half] * piece]
                sums[block] = sums[block] + jnp.concatenate(term, axis=0)
    for block in range(GRAINS - 1):
        rows = [
            jnp.sum(across[j], axis=0, keepdims=True)
            for j in range(GRAIN * block, GRAIN * (block + 1))
        ]
        sums[block] = sums[block] + jnp.concatenate(rows, axis=0)
    return jnp.concatenate(sums, axis=0)


def state_body(source_ref, state_ref, tok_ref, src_ref, feats_ref):
    for block in range(BLOCKS):
        source = source_ref[block]
        tok_ref[block] = source.astype(BF16)
        src_ref[block] = source.T.astype(BF16)
    state_ref[...] = jnp.zeros_like(state_ref)

    def step(tile, carry):
        xt = jnp.concatenate([src_ref[2 * tile, :HD], src_ref[2 * tile + 1, :HD]], axis=1)
        write_features(xt.astype(F32), 1.0, feats_ref)
        tok = jnp.concatenate([tok_ref[2 * tile], tok_ref[2 * tile + 1]], axis=0)
        values = tok[:, HD:]
        zeros = jnp.zeros_like(values)
        state_ref[...] += dot(
            feats_ref[:HALF, :], jnp.concatenate([values, zeros], axis=1)
        ) + dot(feats_ref[HALF:, :], jnp.concatenate([zeros, values], axis=1))
        return carry

    lax.fori_loop(0, BLOCKS // 2, step, 0)


def local_body(tiles, first_tile, tok_ref, src_ref, target_ref, local_ref, *out_refs):
    core = lax.axis_index("core")
    width = 2 * TB
    sign = 1 - 2 * core
    out_ref = target_ref
    if out_refs:
        out_ref = out_refs[0]
        for block in range(BLOCKS):
            out_ref[block] = target_ref[block].T.astype(BF16)
    local_ref[...] = jnp.zeros_like(local_ref)
    ahead = lax.broadcasted_iota(jnp.int32, (width, width), 0) - lax.broadcasted_iota(
        jnp.int32, (width, width), 1
    )

    def outer(number, carry):
        tile = first_tile + number
        target = jnp.concatenate([out_ref[2 * tile], out_ref[2 * tile + 1]], axis=1)
        zeros = jnp.zeros((HD, width), BF16)
        score_rhs = jnp.concatenate([target[:HD], zeros], axis=0)
        value_rhs = jnp.concatenate([zeros, target[HD:]], axis=0)

        def inner(source, carry):
            tok = jnp.concatenate([tok_ref[2 * source], tok_ref[2 * source + 1]], axis=0)
            scores = dot(tok, score_rhs)
            products = dot(tok, value_rhs)
            keep = (ahead + (source - tile) * width) * sign <= 0
            scaled = jnp.where(keep, scores, 0.0) * (1.0 / HD)
            attn = (scaled * scaled).astype(BF16)
            pgrad = (scaled * products * (2.0 / HD)).astype(BF16)
            left = jnp.concatenate([src_ref[2 * source], src_ref[2 * source + 1]], axis=1)
            local_ref[number, :HD] += dot(left[:HD], pgrad)
            local_ref[number, HD:] += dot(left[HD:], attn)
            return carry

        first = jnp.where(core == 0, 0, tile)
        last = jnp.where(core == 0, tile + 1, BLOCKS // 2)
        lax.fori_loop(first, last, inner, 0)
        return carry

    lax.fori_loop(0, tiles, outer, 0)


def scan_body(parts_ref, unused_ref, sums_ref):
    core = lax.axis_index("core")
    count = parts_ref.shape[0]

    def step(number, total):
        place = number + core * (count - 1 - 2 * number)
        sums_ref[place] = total
        return total + parts_ref[place]

    lax.fori_loop(0, count, step, jnp.zeros(parts_ref.shape[1:], F32))


def grads_body(state_ref, out_ref, early_ref, late_ref, grads_ref, rows_ref, cols_ref, wide_ref, feats_ref):
    rows_ref[...] = state_ref[...].astype(BF16)
    for start in range(0, HALF, TB):
        stop = min(start + TB, HALF)
        part = state_ref[start:stop, :]
        if stop - start < TB:
            part = jnp.concatenate([part, jnp.zeros((TB - stop + start, TB), F32)], axis=0)
        cols_ref[:, start:stop] = part.T[:, : stop - start].astype(BF16)

    def step(tile, carry):
        target = jnp.concatenate([out_ref[2 * tile], out_ref[2 * tile + 1]], axis=1)
        xt = target[:HD].astype(F32)
        zeros = jnp.zeros((HD, 2 * TB), BF16)
        wide_ref[:HALF] = dot(rows_ref[...], jnp.concatenate([target[HD:], zeros], axis=0))
        wide_ref[HALF:] = dot(rows_ref[...], jnp.concatenate([zeros, target[HD:]], axis=0))
        write_features(xt, 2.0, feats_ref)
        values = dot(cols_ref[:HD, :], feats_ref[:HALF]) + dot(cols_ref[HD:, :], feats_ref[HALF:])
        local = jnp.where(tile < 2, early_ref[tile % 2], late_ref[tile % 2])
        result = local + jnp.concatenate(
            [chain_back(xt, wide_ref) * (2.0 / (HD * HD)), values * (1.0 / (HD * HD))], axis=0
        )
        grads_ref[2 * tile] = result[:, :TB].T
        grads_ref[2 * tile + 1] = result[:, TB:].T
        return carry

    lax.fori_loop(0, BLOCKS // 2, step, 0)


def project_body(grads_ref, wq_ref, wk_ref, wv_ref, out_ref):
    query = jnp.concatenate([grads_ref[2 * h][:, :HD] for h in range(CHIPS)], axis=1)
    key = jnp.concatenate([grads_ref[2 * h + 1][:, :HD] for h in range(CHIPS)], axis=1)
    value = jnp.concatenate([grads_ref[2 * h + 1][:, HD:] for h in range(CHIPS)], axis=1)
    query, key, value = query.astype(BF16), key.astype(BF16), value.astype(BF16)
    width = out_ref.shape[2]
    for place in range(out_ref.shape[0]):
        cols = slice(place * width, (place + 1) * width)
        out_ref[place] = (
            dot(query, wq_ref[:, cols]) + dot(key, wk_ref[:, cols]) + dot(value, wv_ref[:, cols])
        )


def on_device(queries, keys, values, out_grad, w_query, w_key, w_value):
    shape = jax.ShapeDtypeStruct
    groups = lax.axis_size("x") * lax.axis_size("zg")
    packed = call(
        pack_body,
        shape((BLOCKS, TB, TB), F32),
        (queries, keys, values, out_grad),
        "pack",
        limit=None,
        flops=1 << 20,
        nbytes=1 << 20,
    )
    source = lax.all_to_all(packed, ("zc", "core"), 0, 0, tiled=True)
    target = lax.ppermute(source, "core", [(0, 1), (1, 0)])
    blocks = shape((BLOCKS, TB, TB), BF16)
    state, tok, src = call(
        state_body,
        (shape((HALF, TB), F32), blocks, blocks),
        (source,),
        "state",
        scratch=[pltpu.VMEM((2 * HALF, 2 * TB), BF16)],
        flops=4 << 30,
        nbytes=3 << 20,
    )
    parts = lax.all_to_all(
        state.reshape(groups, 1, HALF * TB // groups), ("x", "zg"), 0, 0, tiled=True
    )
    tiles = BLOCKS // 4
    halves = shape((tiles, TB, 2 * TB), F32)
    early, out = call(
        functools.partial(local_body, tiles, 0),
        (halves, blocks),
        (tok, src, target),
        "early",
        flops=2 << 30,
        nbytes=1 << 20,
    )
    sums = call(
        scan_body, shape(parts.shape, F32), (parts, early), "scan", flops=1 << 20, nbytes=1 << 20
    )
    before = lax.all_to_all(sums, ("x", "zg"), 0, 0, tiled=True).reshape(HALF, TB)
    (late,) = call(
        functools.partial(local_body, tiles, tiles),
        (halves,),
        (tok, src, out),
        "late",
        flops=2 << 30,
        nbytes=1 << 20,
    )
    grads = call(
        grads_body,
        shape((BLOCKS, TB, TB), F32),
        (before, out, early, late),
        "grads",
        scratch=[
            pltpu.VMEM((HALF, TB), BF16),
            pltpu.VMEM((TB, HALF), BF16),
            pltpu.VMEM((2 * HALF, 2 * TB), F32),
            pltpu.VMEM((2 * HALF, 2 * TB), BF16),
        ],
        flops=4 << 30,
        nbytes=3 << 20,
    )
    mine = lax.all_to_all(grads, ("zc", "core"), 0, 0, tiled=True)
    heads = lax.axis_size("y")
    partial_sum = call(
        project_body,
        shape((heads, TB, w_query.shape[1] // heads), F32),
        (mine, w_query, w_key, w_value),
        "project",
        flops=1 << 29,
        nbytes=4 << 20,
    )
    pieces = lax.all_to_all(partial_sum, "y", 0, 0, tiled=True)
    return jnp.sum(pieces, axis=0).astype(BF16)


def solution(mesh):
    seq, head = mesh.devices.shape
    cols = 4 if seq >= 128 else 2
    grid = Mesh(
        mesh.devices.reshape(seq // (cols * 8), cols, CHIPS, 2, head),
        ("x", "zg", "zc", "core", "y"),
    )
    tokens = ("x", "zg", "zc", "core")
    placed = (P(tokens, "y"),) * 4 + (P("y", None),) * 3
    return jax.shard_map(
        on_device, mesh=grid, in_specs=placed, out_specs=P(tokens, "y"), check_vma=False
    )
```

```python
import functools

import jax
import jax.numpy as jnp
from jax import lax
from jax.experimental import pallas as pl
from jax.experimental.pallas import tpu as pltpu
from jax.sharding import Mesh
from jax.sharding import PartitionSpec as P

HD = 64
TB = 128
CHIPS = 4
BLOCKS = 8
GRAIN = 8
GRAINS = HD // GRAIN
HALF = 1040


def row_tiles():
    off = [
        [("off", j, other) for j in range(GRAIN * block, GRAIN * (block + 1)) for other in range(block + 1, GRAINS)]
        for block in range(GRAINS)
    ]
    ring = [[("ring", block, step) for step in range(GRAIN // 2)] for block in range(GRAINS)]
    left = [("left", block, block + 1) for block in range(0, GRAINS, 2)]
    first = off[0] + off[1] + sum(ring[:6], []) + left[:2]
    return first + sum(off[2:], []) + sum(ring[6:], []) + left[2:]


TILES = row_tiles()
assert len(TILES) * GRAIN == 2 * HALF
VMEM = pl.BlockSpec(memory_space=pltpu.VMEM)
F32 = jnp.float32
BF16 = jnp.bfloat16


def call(body, out_shape, args, name, scratch=(), flops=0, nbytes=0, limit=24 << 20):
    return pl.pallas_call(
        body,
        out_shape=out_shape,
        in_specs=[VMEM] * len(args),
        out_specs=jax.tree.map(lambda unused: VMEM, out_shape),
        scratch_shapes=list(scratch),
        name=name,
        compiler_params=pltpu.CompilerParams(vmem_limit_bytes=limit),
        cost_estimate=pl.CostEstimate(flops=flops, bytes_accessed=nbytes, transcendentals=0),
    )(*args)


def dot(a, b):
    return jnp.dot(a, b, preferred_element_type=F32)


def pack_body(q_ref, k_ref, v_ref, g_ref, out_ref):
    for head in range(CHIPS):
        cols = slice(head * HD, (head + 1) * HD)
        out_ref[2 * head] = jnp.concatenate([k_ref[:, cols], v_ref[:, cols]], axis=1).astype(F32)
        out_ref[2 * head + 1] = jnp.concatenate([q_ref[:, cols], g_ref[:, cols]], axis=1).astype(F32)


def turned(grain, step):
    return jnp.concatenate([grain[step:], grain[:step]], axis=0) if step else grain


def write_features(xt, factor, feats_ref):
    grains = [xt[GRAIN * block : GRAIN * (block + 1)] for block in range(GRAINS)]
    twice = [grain * factor for grain in grains] if factor != 1.0 else grains
    half = GRAIN // 2
    tiles = []
    for kind, one, two in TILES:
        if kind == "off":
            tiles.append(xt[one : one + 1] * twice[two])
        elif kind == "ring":
            tiles.append(grains[one] * turned(twice[one] if two else grains[one], two))
        else:
            pieces = [grains[block][:half] * twice[block][half:] for block in (one, two)]
            tiles.append(jnp.concatenate(pieces, axis=0))
    for place in range(0, len(tiles), 2):
        rows = slice(GRAIN * place, GRAIN * (place + 2))
        feats_ref[rows, :] = jnp.concatenate(tiles[place : place + 2], axis=0).astype(BF16)


def chain_back(xt, wide_ref):
    grains = [xt[GRAIN * block : GRAIN * (block + 1)] for block in range(GRAINS)]
    sums = [jnp.zeros(grains[0].shape, F32) for unused in range(GRAINS)]
    across = {}
    half = GRAIN // 2
    for place, (kind, one, two) in enumerate(TILES):
        wide = wide_ref[GRAIN * place : GRAIN * (place + 1)]
        if kind == "off":
            sums[two] = sums[two] + xt[one : one + 1] * wide
            term = grains[two] * wide
            across[one] = across[one] + term if one in across else term
        elif kind == "ring":
            sums[one] = sums[one] + turned(grains[one], two) * wide
            if two:
                sums[one] = sums[one] + turned(grains[one] * wide, GRAIN - two)
        else:
            for number, block in enumerate((one, two)):
                piece = wide[half * number : half * (number + 1)]
                term = [grains[block][half:] * piece, grains[block][:half] * piece]
                sums[block] = sums[block] + jnp.concatenate(term, axis=0)
    for block in range(GRAINS - 1):
        rows = [
            jnp.sum(across[j], axis=0, keepdims=True)
            for j in range(GRAIN * block, GRAIN * (block + 1))
        ]
        sums[block] = sums[block] + jnp.concatenate(rows, axis=0)
    return jnp.concatenate(sums, axis=0)


def state_body(source_ref, state_ref, tok_ref, src_ref, *feats_refs):
    for tile in range(BLOCKS // 2):
        feats_ref = feats_refs[tile % len(feats_refs)]
        for block in (2 * tile, 2 * tile + 1):
            source = source_ref[block]
            tok_ref[block] = source.astype(BF16)
            src_ref[block] = source.T.astype(BF16)
        xt = jnp.concatenate([src_ref[2 * tile, :HD], src_ref[2 * tile + 1, :HD]], axis=1)
        write_features(xt.astype(F32), 1.0, feats_ref)
        tok = jnp.concatenate([tok_ref[2 * tile], tok_ref[2 * tile + 1]], axis=0)
        values = tok[:, HD:]
        zeros = jnp.zeros_like(values)
        part = dot(feats_ref[:HALF, :], jnp.concatenate([values, zeros], axis=1)) + dot(
            feats_ref[HALF:, :], jnp.concatenate([zeros, values], axis=1)
        )
        state_ref[...] = part if tile == 0 else state_ref[...] + part


def local_body(tok_ref, src_ref, target_ref, local_ref, out_ref):
    core = lax.axis_index("core")
    tiles = BLOCKS // 2
    width = 2 * TB
    sign = 1 - 2 * core
    for block in range(BLOCKS):
        out_ref[block] = target_ref[block].T.astype(BF16)
    local_ref[...] = jnp.zeros_like(local_ref)
    ahead = lax.broadcasted_iota(jnp.int32, (width, width), 0) - lax.broadcasted_iota(
        jnp.int32, (width, width), 1
    )

    def outer(tile, carry):
        target = jnp.concatenate([out_ref[2 * tile], out_ref[2 * tile + 1]], axis=1)
        zeros = jnp.zeros((HD, width), BF16)
        score_rhs = jnp.concatenate([target[:HD], zeros], axis=0)
        value_rhs = jnp.concatenate([zeros, target[HD:]], axis=0)

        def inner(source, carry):
            tok = jnp.concatenate([tok_ref[2 * source], tok_ref[2 * source + 1]], axis=0)
            scores = dot(tok, score_rhs)
            products = dot(tok, value_rhs)
            keep = (ahead + (source - tile) * width) * sign <= 0
            scaled = jnp.where(keep, scores, 0.0) * (1.0 / HD)
            attn = (scaled * scaled).astype(BF16)
            pgrad = (scaled * products * (2.0 / HD)).astype(BF16)
            left = jnp.concatenate([src_ref[2 * source], src_ref[2 * source + 1]], axis=1)
            local_ref[tile, :HD] += dot(left[:HD], pgrad)
            local_ref[tile, HD:] += dot(left[HD:], attn)
            return carry

        first = jnp.where(core == 0, 0, tile)
        last = jnp.where(core == 0, tile + 1, tiles)
        lax.fori_loop(first, last, inner, 0)
        return carry

    lax.fori_loop(0, tiles, outer, 0)


def scan_body(parts_ref, sums_ref):
    core = lax.axis_index("core")
    count = parts_ref.shape[0]

    def step(number, total):
        place = number + core * (count - 1 - 2 * number)
        sums_ref[place] = total
        return total + parts_ref[place]

    lax.fori_loop(0, count, step, jnp.zeros(parts_ref.shape[1:], F32))


def grads_body(state_ref, out_ref, local_ref, grads_ref, rows_ref, cols_ref, *tile_refs):
    rows_ref[...] = state_ref[...].astype(BF16)
    for start in range(0, HALF, TB):
        stop = min(start + TB, HALF)
        part = state_ref[start:stop, :]
        if stop - start < TB:
            part = jnp.concatenate([part, jnp.zeros((TB - stop + start, TB), F32)], axis=0)
        cols_ref[:, start:stop] = part.T[:, : stop - start].astype(BF16)
    zeros = jnp.zeros((HD, 2 * TB), BF16)
    for tile in range(BLOCKS // 2):
        wide_ref, feats_ref = tile_refs[tile % 2], tile_refs[2 + tile % 2]
        target = jnp.concatenate([out_ref[2 * tile], out_ref[2 * tile + 1]], axis=1)
        wide_ref[:HALF] = dot(rows_ref[...], jnp.concatenate([target[HD:], zeros], axis=0))
        wide_ref[HALF:] = dot(rows_ref[...], jnp.concatenate([zeros, target[HD:]], axis=0))
        xt = target[:HD].astype(F32)
        write_features(xt, 2.0, feats_ref)
        values = dot(cols_ref[:HD, :], feats_ref[:HALF]) + dot(cols_ref[HD:, :], feats_ref[HALF:])
        back = chain_back(xt, wide_ref)
        result = local_ref[tile] + jnp.concatenate(
            [back * (2.0 / (HD * HD)), values * (1.0 / (HD * HD))], axis=0
        )
        grads_ref[2 * tile] = result[:, :TB].T
        grads_ref[2 * tile + 1] = result[:, TB:].T


def project_body(grads_ref, wq_ref, wk_ref, wv_ref, out_ref):
    query = jnp.concatenate([grads_ref[2 * h][:, :HD] for h in range(CHIPS)], axis=1)
    key = jnp.concatenate([grads_ref[2 * h + 1][:, :HD] for h in range(CHIPS)], axis=1)
    value = jnp.concatenate([grads_ref[2 * h + 1][:, HD:] for h in range(CHIPS)], axis=1)
    query, key, value = query.astype(BF16), key.astype(BF16), value.astype(BF16)
    width = out_ref.shape[2]
    for place in range(out_ref.shape[0]):
        cols = slice(place * width, (place + 1) * width)
        out_ref[place] = (
            dot(query, wq_ref[:, cols]) + dot(key, wk_ref[:, cols]) + dot(value, wv_ref[:, cols])
        )


def on_device(queries, keys, values, out_grad, w_query, w_key, w_value):
    shape = jax.ShapeDtypeStruct
    groups = lax.axis_size("x") * lax.axis_size("zg")
    packed = call(
        pack_body,
        shape((BLOCKS, TB, TB), F32),
        (queries, keys, values, out_grad),
        "pack",
        limit=None,
        flops=1 << 20,
        nbytes=1 << 20,
    )
    source = lax.all_to_all(packed, ("zc", "core"), 0, 0, tiled=True)
    target = lax.ppermute(source, "core", [(0, 1), (1, 0)])
    blocks = shape((BLOCKS, TB, TB), BF16)
    state, tok, src = call(
        state_body,
        (shape((HALF, TB), F32), blocks, blocks),
        (source,),
        "state",
        scratch=[pltpu.VMEM((2 * HALF, 2 * TB), BF16)] * 2,
        flops=4 << 30,
        nbytes=3 << 20,
    )
    parts = lax.all_to_all(
        state.reshape(groups, 1, HALF * TB // groups), ("x", "zg"), 0, 0, tiled=True
    )
    sums = call(
        scan_body, shape(parts.shape, F32), (parts,), "scan", flops=1 << 20, nbytes=1 << 20
    )
    before = lax.all_to_all(sums, ("x", "zg"), 0, 0, tiled=True).reshape(HALF, TB)
    local, out = call(
        local_body,
        (shape((BLOCKS // 2, TB, 2 * TB), F32), blocks),
        (tok, src, target),
        "local",
        flops=4 << 30,
        nbytes=1 << 20,
    )
    grads = call(
        grads_body,
        shape((BLOCKS, TB, TB), F32),
        (before, out, local),
        "grads",
        scratch=[
            pltpu.VMEM((HALF, TB), BF16),
            pltpu.VMEM((TB, HALF), BF16),
            pltpu.VMEM((2 * HALF, 2 * TB), F32),
            pltpu.VMEM((2 * HALF, 2 * TB), F32),
            pltpu.VMEM((2 * HALF, 2 * TB), BF16),
            pltpu.VMEM((2 * HALF, 2 * TB), BF16),
        ],
        flops=4 << 30,
        nbytes=3 << 20,
    )
    mine = lax.all_to_all(grads, ("zc", "core"), 0, 0, tiled=True)
    heads = lax.axis_size("y")
    partial_sum = call(
        project_body,
        shape((heads, TB, w_query.shape[1] // heads), F32),
        (mine, w_query, w_key, w_value),
        "project",
        flops=1 << 29,
        nbytes=4 << 20,
    )
    pieces = lax.all_to_all(partial_sum, "y", 0, 0, tiled=True)
    return jnp.sum(pieces, axis=0).astype(BF16)


def solution(mesh):
    seq, head = mesh.devices.shape
    cols = 4 if seq >= 128 else 2
    grid = Mesh(
        mesh.devices.reshape(seq // (cols * 8), cols, CHIPS, 2, head),
        ("x", "zg", "zc", "core", "y"),
    )
    tokens = ("x", "zg", "zc", "core")
    placed = (P(tokens, "y"),) * 4 + (P("y", None),) * 3
    return jax.shard_map(
        on_device, mesh=grid, in_specs=placed, out_specs=P(tokens, "y"), check_vma=False
    )
```

```python
import functools

import jax
import jax.numpy as jnp
from jax import lax
from jax.experimental import pallas as pl
from jax.experimental.pallas import tpu as pltpu
from jax.sharding import Mesh
from jax.sharding import PartitionSpec as P

HD = 64
TB = 128
CHIPS = 4
BLOCKS = 8
GRAIN = 8
GRAINS = HD // GRAIN
HALF = 1040


def row_tiles():
    off = [
        [("off", j, other) for j in range(GRAIN * block, GRAIN * (block + 1)) for other in range(block + 1, GRAINS)]
        for block in range(GRAINS)
    ]
    ring = [[("ring", block, step) for step in range(GRAIN // 2)] for block in range(GRAINS)]
    left = [("left", block, block + 1) for block in range(0, GRAINS, 2)]
    first = off[0] + off[1] + sum(ring[:6], []) + left[:2]
    return first + sum(off[2:], []) + sum(ring[6:], []) + left[2:]


TILES = row_tiles()
assert len(TILES) * GRAIN == 2 * HALF
VMEM = pl.BlockSpec(memory_space=pltpu.VMEM)
F32 = jnp.float32
BF16 = jnp.bfloat16


def call(body, out_shape, args, name, scratch=(), flops=0, nbytes=0, limit=24 << 20):
    return pl.pallas_call(
        body,
        out_shape=out_shape,
        in_specs=[VMEM] * len(args),
        out_specs=jax.tree.map(lambda unused: VMEM, out_shape),
        scratch_shapes=list(scratch),
        name=name,
        compiler_params=pltpu.CompilerParams(vmem_limit_bytes=limit),
        cost_estimate=pl.CostEstimate(flops=flops, bytes_accessed=nbytes, transcendentals=0),
    )(*args)


def dot(a, b):
    return jnp.dot(a, b, preferred_element_type=F32)


def pack_body(q_ref, k_ref, v_ref, g_ref, out_ref):
    for head in range(CHIPS):
        cols = slice(head * HD, (head + 1) * HD)
        out_ref[2 * head] = jnp.concatenate([k_ref[:, cols], v_ref[:, cols]], axis=1).astype(F32)
        out_ref[2 * head + 1] = jnp.concatenate([q_ref[:, cols], g_ref[:, cols]], axis=1).astype(F32)


def turned(grain, step):
    return jnp.concatenate([grain[step:], grain[:step]], axis=0) if step else grain


def write_features(xt, factor, feats_ref):
    grains = [xt[GRAIN * block : GRAIN * (block + 1)] for block in range(GRAINS)]
    twice = [grain * factor for grain in grains] if factor != 1.0 else grains
    half = GRAIN // 2
    tiles = []
    for kind, one, two in TILES:
        if kind == "off":
            tiles.append(xt[one : one + 1] * twice[two])
        elif kind == "ring":
            tiles.append(grains[one] * turned(twice[one] if two else grains[one], two))
        else:
            pieces = [grains[block][:half] * twice[block][half:] for block in (one, two)]
            tiles.append(jnp.concatenate(pieces, axis=0))
    for place in range(0, len(tiles), 2):
        rows = slice(GRAIN * place, GRAIN * (place + 2))
        feats_ref[rows, :] = jnp.concatenate(tiles[place : place + 2], axis=0).astype(BF16)


def chain_back(xt, wide_ref):
    grains = [xt[GRAIN * block : GRAIN * (block + 1)] for block in range(GRAINS)]
    sums = [jnp.zeros(grains[0].shape, F32) for unused in range(GRAINS)]
    across = {}
    half = GRAIN // 2
    for place, (kind, one, two) in enumerate(TILES):
        wide = wide_ref[GRAIN * place : GRAIN * (place + 1)]
        if kind == "off":
            sums[two] = sums[two] + xt[one : one + 1] * wide
            term = grains[two] * wide
            across[one] = across[one] + term if one in across else term
        elif kind == "ring":
            sums[one] = sums[one] + turned(grains[one], two) * wide
            if two:
                sums[one] = sums[one] + turned(grains[one] * wide, GRAIN - two)
        else:
            for number, block in enumerate((one, two)):
                piece = wide[half * number : half * (number + 1)]
                term = [grains[block][half:] * piece, grains[block][:half] * piece]
                sums[block] = sums[block] + jnp.concatenate(term, axis=0)
    for block in range(GRAINS - 1):
        rows = [
            jnp.sum(across[j], axis=0, keepdims=True)
            for j in range(GRAIN * block, GRAIN * (block + 1))
        ]
        sums[block] = sums[block] + jnp.concatenate(rows, axis=0)
    return jnp.concatenate(sums, axis=0)


def state_body(source_ref, state_ref, tok_ref, src_ref, *feats_refs):
    for tile in range(BLOCKS // 2):
        feats_ref = feats_refs[tile % len(feats_refs)]
        for block in (2 * tile, 2 * tile + 1):
            source = source_ref[block]
            tok_ref[block] = source.astype(BF16)
            src_ref[block] = source.T.astype(BF16)
        xt = jnp.concatenate([src_ref[2 * tile, :HD], src_ref[2 * tile + 1, :HD]], axis=1)
        write_features(xt.astype(F32), 1.0, feats_ref)
        tok = jnp.concatenate([tok_ref[2 * tile], tok_ref[2 * tile + 1]], axis=0)
        values = tok[:, HD:]
        zeros = jnp.zeros_like(values)
        part = dot(feats_ref[:HALF, :], jnp.concatenate([values, zeros], axis=1)) + dot(
            feats_ref[HALF:, :], jnp.concatenate([zeros, values], axis=1)
        )
        state_ref[...] = part if tile == 0 else state_ref[...] + part


def local_body(tok_ref, src_ref, target_ref, local_ref, out_ref):
    core = lax.axis_index("core")
    tiles = BLOCKS // 2
    width = 2 * TB
    sign = 1 - 2 * core
    for block in range(BLOCKS):
        out_ref[block] = target_ref[block].T.astype(BF16)
    local_ref[...] = jnp.zeros_like(local_ref)
    ahead = lax.broadcasted_iota(jnp.int32, (width, width), 0) - lax.broadcasted_iota(
        jnp.int32, (width, width), 1
    )

    def outer(tile, carry):
        target = jnp.concatenate([out_ref[2 * tile], out_ref[2 * tile + 1]], axis=1)
        zeros = jnp.zeros((HD, width), BF16)
        score_rhs = jnp.concatenate([target[:HD], zeros], axis=0)
        value_rhs = jnp.concatenate([zeros, target[HD:]], axis=0)

        def inner(source, carry):
            tok = jnp.concatenate([tok_ref[2 * source], tok_ref[2 * source + 1]], axis=0)
            scores = dot(tok, score_rhs)
            products = dot(tok, value_rhs)
            keep = (ahead + (source - tile) * width) * sign <= 0
            scaled = jnp.where(keep, scores, 0.0) * (1.0 / HD)
            attn = (scaled * scaled).astype(BF16)
            pgrad = (scaled * products * (2.0 / HD)).astype(BF16)
            left = jnp.concatenate([src_ref[2 * source], src_ref[2 * source + 1]], axis=1)
            local_ref[tile, :HD] += dot(left[:HD], pgrad)
            local_ref[tile, HD:] += dot(left[HD:], attn)
            return carry

        first = jnp.where(core == 0, 0, tile)
        last = jnp.where(core == 0, tile + 1, tiles)
        lax.fori_loop(first, last, inner, 0)
        return carry

    lax.fori_loop(0, tiles, outer, 0)


def scan_body(parts_ref, sums_ref):
    core = lax.axis_index("core")
    count = parts_ref.shape[0]
    cols, rows = lax.axis_size("zg"), lax.axis_size("x")

    def step(number, total):
        segment = number + core * (count - 1 - 2 * number)
        place = lax.rem(segment, cols) * rows + lax.div(segment, cols)
        sums_ref[place] = total
        return total + parts_ref[place]

    lax.fori_loop(0, count, step, jnp.zeros(parts_ref.shape[1:], F32))


def grads_body(state_ref, out_ref, local_ref, grads_ref, rows_ref, cols_ref, *tile_refs):
    rows_ref[...] = state_ref[...].astype(BF16)
    for start in range(0, HALF, TB):
        stop = min(start + TB, HALF)
        part = state_ref[start:stop, :]
        if stop - start < TB:
            part = jnp.concatenate([part, jnp.zeros((TB - stop + start, TB), F32)], axis=0)
        cols_ref[:, start:stop] = part.T[:, : stop - start].astype(BF16)
    zeros = jnp.zeros((HD, 2 * TB), BF16)
    for tile in range(BLOCKS // 2):
        wide_ref, feats_ref = tile_refs[tile % 2], tile_refs[2 + tile % 2]
        target = jnp.concatenate([out_ref[2 * tile], out_ref[2 * tile + 1]], axis=1)
        wide_ref[:HALF] = dot(rows_ref[...], jnp.concatenate([target[HD:], zeros], axis=0))
        wide_ref[HALF:] = dot(rows_ref[...], jnp.concatenate([zeros, target[HD:]], axis=0))
        xt = target[:HD].astype(F32)
        write_features(xt, 2.0, feats_ref)
        values = dot(cols_ref[:HD, :], feats_ref[:HALF]) + dot(cols_ref[HD:, :], feats_ref[HALF:])
        back = chain_back(xt, wide_ref)
        result = local_ref[tile] + jnp.concatenate(
            [back * (2.0 / (HD * HD)), values * (1.0 / (HD * HD))], axis=0
        )
        grads_ref[2 * tile] = result[:, :TB].T
        grads_ref[2 * tile + 1] = result[:, TB:].T


def project_body(grads_ref, wq_ref, wk_ref, wv_ref, out_ref):
    query = jnp.concatenate([grads_ref[2 * h][:, :HD] for h in range(CHIPS)], axis=1)
    key = jnp.concatenate([grads_ref[2 * h + 1][:, :HD] for h in range(CHIPS)], axis=1)
    value = jnp.concatenate([grads_ref[2 * h + 1][:, HD:] for h in range(CHIPS)], axis=1)
    query, key, value = query.astype(BF16), key.astype(BF16), value.astype(BF16)
    width = out_ref.shape[2]
    for place in range(out_ref.shape[0]):
        cols = slice(place * width, (place + 1) * width)
        out_ref[place] = (
            dot(query, wq_ref[:, cols]) + dot(key, wk_ref[:, cols]) + dot(value, wv_ref[:, cols])
        )


def on_device(queries, keys, values, out_grad, w_query, w_key, w_value):
    shape = jax.ShapeDtypeStruct
    groups = lax.axis_size("x") * lax.axis_size("zg")
    packed = call(
        pack_body,
        shape((BLOCKS, TB, TB), F32),
        (queries, keys, values, out_grad),
        "pack",
        limit=None,
        flops=1 << 20,
        nbytes=1 << 20,
    )
    source = lax.all_to_all(packed, ("zc", "core"), 0, 0, tiled=True)
    target = lax.ppermute(source, "core", [(0, 1), (1, 0)])
    blocks = shape((BLOCKS, TB, TB), BF16)
    state, tok, src = call(
        state_body,
        (shape((HALF, TB), F32), blocks, blocks),
        (source,),
        "state",
        scratch=[pltpu.VMEM((2 * HALF, 2 * TB), BF16)] * 2,
        flops=4 << 30,
        nbytes=3 << 20,
    )
    parts = lax.all_to_all(
        state.reshape(groups, 1, HALF * TB // groups), ("zg", "x"), 0, 0, tiled=True
    )
    sums = call(
        scan_body, shape(parts.shape, F32), (parts,), "scan", flops=1 << 20, nbytes=1 << 20
    )
    before = lax.all_to_all(sums, ("zg", "x"), 0, 0, tiled=True).reshape(HALF, TB)
    local, out = call(
        local_body,
        (shape((BLOCKS // 2, TB, 2 * TB), F32), blocks),
        (tok, src, target),
        "local",
        flops=4 << 30,
        nbytes=1 << 20,
    )
    grads = call(
        grads_body,
        shape((BLOCKS, TB, TB), F32),
        (before, out, local),
        "grads",
        scratch=[
            pltpu.VMEM((HALF, TB), BF16),
            pltpu.VMEM((TB, HALF), BF16),
            pltpu.VMEM((2 * HALF, 2 * TB), F32),
            pltpu.VMEM((2 * HALF, 2 * TB), F32),
            pltpu.VMEM((2 * HALF, 2 * TB), BF16),
            pltpu.VMEM((2 * HALF, 2 * TB), BF16),
        ],
        flops=4 << 30,
        nbytes=3 << 20,
    )
    mine = lax.all_to_all(grads, ("zc", "core"), 0, 0, tiled=True)
    heads = lax.axis_size("y")
    partial_sum = call(
        project_body,
        shape((heads, TB, w_query.shape[1] // heads), F32),
        (mine, w_query, w_key, w_value),
        "project",
        flops=1 << 29,
        nbytes=4 << 20,
    )
    pieces = lax.all_to_all(partial_sum, "y", 0, 0, tiled=True)
    return jnp.sum(pieces, axis=0).astype(BF16)


def solution(mesh):
    seq, head = mesh.devices.shape
    cols = 4 if seq >= 128 else 2
    grid = Mesh(
        mesh.devices.reshape(seq // (cols * 8), cols, CHIPS, 2, head),
        ("x", "zg", "zc", "core", "y"),
    )
    tokens = ("x", "zg", "zc", "core")
    placed = (P(tokens, "y"),) * 4 + (P("y", None),) * 3
    return jax.shard_map(
        on_device, mesh=grid, in_specs=placed, out_specs=P(tokens, "y"), check_vma=False
    )
```

```python
import functools

import jax
import jax.numpy as jnp
from jax import lax
from jax.experimental import pallas as pl
from jax.experimental.pallas import tpu as pltpu
from jax.sharding import PartitionSpec as P

HD = 64
TB = 128
CHIPS = 4
BLOCKS = 8
GRAIN = 8
GRAINS = HD // GRAIN
HALF = 1040


def row_tiles():
    off = [
        [("off", j, other) for j in range(GRAIN * block, GRAIN * (block + 1)) for other in range(block + 1, GRAINS)]
        for block in range(GRAINS)
    ]
    ring = [[("ring", block, step) for step in range(GRAIN // 2)] for block in range(GRAINS)]
    left = [("left", block, block + 1) for block in range(0, GRAINS, 2)]
    first = off[0] + off[1] + sum(ring[:6], []) + left[:2]
    return first + sum(off[2:], []) + sum(ring[6:], []) + left[2:]


TILES = row_tiles()
assert len(TILES) * GRAIN == 2 * HALF
VMEM = pl.BlockSpec(memory_space=pltpu.VMEM)
F32 = jnp.float32
BF16 = jnp.bfloat16


def call(body, out_shape, args, name, scratch=(), flops=0, nbytes=0, limit=24 << 20):
    return pl.pallas_call(
        body,
        out_shape=out_shape,
        in_specs=[VMEM] * len(args),
        out_specs=jax.tree.map(lambda unused: VMEM, out_shape),
        scratch_shapes=list(scratch),
        name=name,
        compiler_params=pltpu.CompilerParams(vmem_limit_bytes=limit),
        cost_estimate=pl.CostEstimate(flops=flops, bytes_accessed=nbytes, transcendentals=0),
    )(*args)


def dot(a, b):
    return jnp.dot(a, b, preferred_element_type=F32)


def pack_body(q_ref, k_ref, v_ref, g_ref, out_ref):
    for head in range(CHIPS):
        cols = slice(head * HD, (head + 1) * HD)
        out_ref[2 * head] = jnp.concatenate([k_ref[:, cols], v_ref[:, cols]], axis=1).astype(F32)
        out_ref[2 * head + 1] = jnp.concatenate([q_ref[:, cols], g_ref[:, cols]], axis=1).astype(F32)


def turned(grain, step):
    return jnp.concatenate([grain[step:], grain[:step]], axis=0) if step else grain


def write_features(xt, factor, feats_ref):
    grains = [xt[GRAIN * block : GRAIN * (block + 1)] for block in range(GRAINS)]
    twice = [grain * factor for grain in grains] if factor != 1.0 else grains
    half = GRAIN // 2
    tiles = []
    for kind, one, two in TILES:
        if kind == "off":
            tiles.append(xt[one : one + 1] * twice[two])
        elif kind == "ring":
            tiles.append(grains[one] * turned(twice[one] if two else grains[one], two))
        else:
            pieces = [grains[block][:half] * twice[block][half:] for block in (one, two)]
            tiles.append(jnp.concatenate(pieces, axis=0))
    for place in range(0, len(tiles), 2):
        rows = slice(GRAIN * place, GRAIN * (place + 2))
        feats_ref[rows, :] = jnp.concatenate(tiles[place : place + 2], axis=0).astype(BF16)


def chain_back(xt, wide_ref):
    grains = [xt[GRAIN * block : GRAIN * (block + 1)] for block in range(GRAINS)]
    sums = [jnp.zeros(grains[0].shape, F32) for unused in range(GRAINS)]
    across = {}
    half = GRAIN // 2
    for place, (kind, one, two) in enumerate(TILES):
        wide = wide_ref[GRAIN * place : GRAIN * (place + 1)]
        if kind == "off":
            sums[two] = sums[two] + xt[one : one + 1] * wide
            term = grains[two] * wide
            across[one] = across[one] + term if one in across else term
        elif kind == "ring":
            sums[one] = sums[one] + turned(grains[one], two) * wide
            if two:
                sums[one] = sums[one] + turned(grains[one] * wide, GRAIN - two)
        else:
            for number, block in enumerate((one, two)):
                piece = wide[half * number : half * (number + 1)]
                term = [grains[block][half:] * piece, grains[block][:half] * piece]
                sums[block] = sums[block] + jnp.concatenate(term, axis=0)
    for block in range(GRAINS - 1):
        rows = [
            jnp.sum(across[j], axis=0, keepdims=True)
            for j in range(GRAIN * block, GRAIN * (block + 1))
        ]
        sums[block] = sums[block] + jnp.concatenate(rows, axis=0)
    return jnp.concatenate(sums, axis=0)


def state_body(source_ref, state_ref, tok_ref, src_ref, *feats_refs):
    for tile in range(BLOCKS // 2):
        feats_ref = feats_refs[tile % len(feats_refs)]
        for block in (2 * tile, 2 * tile + 1):
            source = source_ref[block]
            tok_ref[block] = source.astype(BF16)
            src_ref[block] = source.T.astype(BF16)
        xt = jnp.concatenate([src_ref[2 * tile, :HD], src_ref[2 * tile + 1, :HD]], axis=1)
        write_features(xt.astype(F32), 1.0, feats_ref)
        tok = jnp.concatenate([tok_ref[2 * tile], tok_ref[2 * tile + 1]], axis=0)
        values = tok[:, HD:]
        zeros = jnp.zeros_like(values)
        part = dot(feats_ref[:HALF, :], jnp.concatenate([values, zeros], axis=1)) + dot(
            feats_ref[HALF:, :], jnp.concatenate([zeros, values], axis=1)
        )
        state_ref[...] = part if tile == 0 else state_ref[...] + part


def local_body(tok_ref, src_ref, target_ref, local_ref, out_ref):
    core = lax.rem(lax.axis_index("seq"), 2)
    tiles = BLOCKS // 2
    width = 2 * TB
    sign = 1 - 2 * core
    for block in range(BLOCKS):
        out_ref[block] = target_ref[block].T.astype(BF16)
    local_ref[...] = jnp.zeros_like(local_ref)
    ahead = lax.broadcasted_iota(jnp.int32, (width, width), 0) - lax.broadcasted_iota(
        jnp.int32, (width, width), 1
    )

    def outer(tile, carry):
        target = jnp.concatenate([out_ref[2 * tile], out_ref[2 * tile + 1]], axis=1)
        zeros = jnp.zeros((HD, width), BF16)
        score_rhs = jnp.concatenate([target[:HD], zeros], axis=0)
        value_rhs = jnp.concatenate([zeros, target[HD:]], axis=0)

        def inner(source, carry):
            tok = jnp.concatenate([tok_ref[2 * source], tok_ref[2 * source + 1]], axis=0)
            scores = dot(tok, score_rhs)
            products = dot(tok, value_rhs)
            keep = (ahead + (source - tile) * width) * sign <= 0
            scaled = jnp.where(keep, scores, 0.0) * (1.0 / HD)
            attn = (scaled * scaled).astype(BF16)
            pgrad = (scaled * products * (2.0 / HD)).astype(BF16)
            left = jnp.concatenate([src_ref[2 * source], src_ref[2 * source + 1]], axis=1)
            local_ref[tile, :HD] += dot(left[:HD], pgrad)
            local_ref[tile, HD:] += dot(left[HD:], attn)
            return carry

        first = jnp.where(core == 0, 0, tile)
        last = jnp.where(core == 0, tile + 1, tiles)
        lax.fori_loop(first, last, inner, 0)
        return carry

    lax.fori_loop(0, tiles, outer, 0)


def scan_body(cols, parts_ref, sums_ref):
    core = lax.rem(lax.axis_index("seq"), 2)
    count = parts_ref.shape[0]
    rows = count // cols

    def step(number, total):
        segment = number + core * (count - 1 - 2 * number)
        column = lax.rem(segment, cols)
        column = jnp.where(core == 0, column, lax.rem(cols - column, cols))
        place = column * rows + lax.div(segment, cols)
        sums_ref[place] = total
        return total + parts_ref[place]

    lax.fori_loop(0, count, step, jnp.zeros(parts_ref.shape[1:], F32))


def grads_body(state_ref, out_ref, local_ref, grads_ref, rows_ref, cols_ref, *tile_refs):
    rows_ref[...] = state_ref[...].astype(BF16)
    for start in range(0, HALF, TB):
        stop = min(start + TB, HALF)
        part = state_ref[start:stop, :]
        if stop - start < TB:
            part = jnp.concatenate([part, jnp.zeros((TB - stop + start, TB), F32)], axis=0)
        cols_ref[:, start:stop] = part.T[:, : stop - start].astype(BF16)
    zeros = jnp.zeros((HD, 2 * TB), BF16)
    for tile in range(BLOCKS // 2):
        wide_ref, feats_ref = tile_refs[tile % 2], tile_refs[2 + tile % 2]
        target = jnp.concatenate([out_ref[2 * tile], out_ref[2 * tile + 1]], axis=1)
        wide_ref[:HALF] = dot(rows_ref[...], jnp.concatenate([target[HD:], zeros], axis=0))
        wide_ref[HALF:] = dot(rows_ref[...], jnp.concatenate([zeros, target[HD:]], axis=0))
        xt = target[:HD].astype(F32)
        write_features(xt, 2.0, feats_ref)
        values = dot(cols_ref[:HD, :], feats_ref[:HALF]) + dot(cols_ref[HD:, :], feats_ref[HALF:])
        back = chain_back(xt, wide_ref)
        result = local_ref[tile] + jnp.concatenate(
            [back * (2.0 / (HD * HD)), values * (1.0 / (HD * HD))], axis=0
        )
        grads_ref[2 * tile] = result[:, :TB].T
        grads_ref[2 * tile + 1] = result[:, TB:].T


def project_body(grads_ref, wq_ref, wk_ref, wv_ref, out_ref):
    query = jnp.concatenate([grads_ref[2 * h][:, :HD] for h in range(CHIPS)], axis=1)
    key = jnp.concatenate([grads_ref[2 * h + 1][:, :HD] for h in range(CHIPS)], axis=1)
    value = jnp.concatenate([grads_ref[2 * h + 1][:, HD:] for h in range(CHIPS)], axis=1)
    query, key, value = query.astype(BF16), key.astype(BF16), value.astype(BF16)
    width = out_ref.shape[2]
    for place in range(out_ref.shape[0]):
        cols = slice(place * width, (place + 1) * width)
        out_ref[place] = (
            dot(query, wq_ref[:, cols]) + dot(key, wk_ref[:, cols]) + dot(value, wv_ref[:, cols])
        )


def segment_groups(rows, cols):
    groups = []
    for place in range(BLOCKS):
        order = [(column if place % 2 == 0 else -column) % cols for column in range(cols)]
        groups.append(
            [(row * cols + column) * BLOCKS + place for column in order for row in range(rows)]
        )
    return groups


def on_device(queries, keys, values, out_grad, w_query, w_key, w_value):
    shape = jax.ShapeDtypeStruct
    devices = lax.axis_size("seq")
    groups = devices // BLOCKS
    cols = 4 if groups >= 16 else 2
    near = [list(range(first, first + BLOCKS)) for first in range(0, devices, BLOCKS)]
    far = segment_groups(groups // cols, cols)
    packed = call(
        pack_body,
        shape((BLOCKS, TB, TB), F32),
        (queries, keys, values, out_grad),
        "pack",
        limit=None,
        flops=1 << 20,
        nbytes=1 << 20,
    )
    source = lax.all_to_all(packed, "seq", 0, 0, axis_index_groups=near, tiled=True)
    target = lax.ppermute(source, "seq", [(place, place ^ 1) for place in range(devices)])
    blocks = shape((BLOCKS, TB, TB), BF16)
    state, tok, src = call(
        state_body,
        (shape((HALF, TB), F32), blocks, blocks),
        (source,),
        "state",
        scratch=[pltpu.VMEM((2 * HALF, 2 * TB), BF16)] * 2,
        flops=4 << 30,
        nbytes=3 << 20,
    )
    parts = lax.all_to_all(
        state.reshape(groups, 1, HALF * TB // groups),
        "seq",
        0,
        0,
        axis_index_groups=far,
        tiled=True,
    )
    sums = call(
        functools.partial(scan_body, cols), shape(parts.shape, F32), (parts,), "scan", flops=1 << 20, nbytes=1 << 20
    )
    before = lax.all_to_all(sums, "seq", 0, 0, axis_index_groups=far, tiled=True)
    before = before.reshape(HALF, TB)
    local, out = call(
        local_body,
        (shape((BLOCKS // 2, TB, 2 * TB), F32), blocks),
        (tok, src, target),
        "local",
        flops=4 << 30,
        nbytes=1 << 20,
    )
    grads = call(
        grads_body,
        shape((BLOCKS, TB, TB), F32),
        (before, out, local),
        "grads",
        scratch=[
            pltpu.VMEM((HALF, TB), BF16),
            pltpu.VMEM((TB, HALF), BF16),
            pltpu.VMEM((2 * HALF, 2 * TB), F32),
            pltpu.VMEM((2 * HALF, 2 * TB), F32),
            pltpu.VMEM((2 * HALF, 2 * TB), BF16),
            pltpu.VMEM((2 * HALF, 2 * TB), BF16),
        ],
        flops=4 << 30,
        nbytes=3 << 20,
    )
    mine = lax.all_to_all(grads, "seq", 0, 0, axis_index_groups=near, tiled=True)
    heads = lax.axis_size("head")
    partial_sum = call(
        project_body,
        shape((heads, TB, w_query.shape[1] // heads), F32),
        (mine, w_query, w_key, w_value),
        "project",
        flops=1 << 29,
        nbytes=4 << 20,
    )
    pieces = lax.all_to_all(partial_sum, "head", 0, 0, tiled=True)
    return jnp.sum(pieces, axis=0).astype(BF16)


def solution(mesh):
    placed = (P("seq", "head"),) * 4 + (P("head", None),) * 3
    return jax.shard_map(
        on_device, mesh=mesh, in_specs=placed, out_specs=P("seq", "head"), check_vma=False
    )
```

```python
import functools

import jax
import jax.numpy as jnp
from jax import lax
from jax.experimental import pallas as pl
from jax.experimental.pallas import tpu as pltpu
from jax.sharding import Mesh
from jax.sharding import PartitionSpec as P

HD = 64
TB = 128
CHIPS = 4
BLOCKS = 8
GRAIN = 8
GRAINS = HD // GRAIN
HALF = 1040


def row_tiles():
    off = [
        [("off", j, other) for j in range(GRAIN * block, GRAIN * (block + 1)) for other in range(block + 1, GRAINS)]
        for block in range(GRAINS)
    ]
    ring = [[("ring", block, step) for step in range(GRAIN // 2)] for block in range(GRAINS)]
    left = [("left", block, block + 1) for block in range(0, GRAINS, 2)]
    first = off[0] + off[1] + sum(ring[:6], []) + left[:2]
    return first + sum(off[2:], []) + sum(ring[6:], []) + left[2:]


TILES = row_tiles()
assert len(TILES) * GRAIN == 2 * HALF
VMEM = pl.BlockSpec(memory_space=pltpu.VMEM)
F32 = jnp.float32
BF16 = jnp.bfloat16


def call(body, out_shape, args, name, scratch=(), flops=0, nbytes=0, limit=24 << 20):
    return pl.pallas_call(
        body,
        out_shape=out_shape,
        in_specs=[VMEM] * len(args),
        out_specs=jax.tree.map(lambda unused: VMEM, out_shape),
        scratch_shapes=list(scratch),
        name=name,
        compiler_params=pltpu.CompilerParams(vmem_limit_bytes=limit),
        cost_estimate=pl.CostEstimate(flops=flops, bytes_accessed=nbytes, transcendentals=0),
    )(*args)


def dot(a, b):
    return jnp.dot(a, b, preferred_element_type=F32)


def pack_body(q_ref, k_ref, v_ref, g_ref, out_ref):
    for head in range(CHIPS):
        cols = slice(head * HD, (head + 1) * HD)
        out_ref[2 * head] = jnp.concatenate([k_ref[:, cols], v_ref[:, cols]], axis=1).astype(F32)
        out_ref[2 * head + 1] = jnp.concatenate([q_ref[:, cols], g_ref[:, cols]], axis=1).astype(F32)


def turned(grain, step):
    return jnp.concatenate([grain[step:], grain[:step]], axis=0) if step else grain


def write_features(xt, factor, feats_ref):
    grains = [xt[GRAIN * block : GRAIN * (block + 1)] for block in range(GRAINS)]
    twice = [grain * factor for grain in grains] if factor != 1.0 else grains
    half = GRAIN // 2
    tiles = []
    for kind, one, two in TILES:
        if kind == "off":
            tiles.append(xt[one : one + 1] * twice[two])
        elif kind == "ring":
            tiles.append(grains[one] * turned(twice[one] if two else grains[one], two))
        else:
            pieces = [grains[block][:half] * twice[block][half:] for block in (one, two)]
            tiles.append(jnp.concatenate(pieces, axis=0))
    for place in range(0, len(tiles), 2):
        rows = slice(GRAIN * place, GRAIN * (place + 2))
        feats_ref[rows, :] = jnp.concatenate(tiles[place : place + 2], axis=0).astype(BF16)


def chain_back(xt, wide_ref):
    grains = [xt[GRAIN * block : GRAIN * (block + 1)] for block in range(GRAINS)]
    sums = [jnp.zeros(grains[0].shape, F32) for unused in range(GRAINS)]
    across = {}
    half = GRAIN // 2
    for place, (kind, one, two) in enumerate(TILES):
        wide = wide_ref[GRAIN * place : GRAIN * (place + 1)]
        if kind == "off":
            sums[two] = sums[two] + xt[one : one + 1] * wide
            term = grains[two] * wide
            across[one] = across[one] + term if one in across else term
        elif kind == "ring":
            sums[one] = sums[one] + turned(grains[one], two) * wide
            if two:
                sums[one] = sums[one] + turned(grains[one] * wide, GRAIN - two)
        else:
            for number, block in enumerate((one, two)):
                piece = wide[half * number : half * (number + 1)]
                term = [grains[block][half:] * piece, grains[block][:half] * piece]
                sums[block] = sums[block] + jnp.concatenate(term, axis=0)
    for block in range(GRAINS - 1):
        rows = [
            jnp.sum(across[j], axis=0, keepdims=True)
            for j in range(GRAIN * block, GRAIN * (block + 1))
        ]
        sums[block] = sums[block] + jnp.concatenate(rows, axis=0)
    return jnp.concatenate(sums, axis=0)


def state_body(source_ref, state_ref, tok_ref, src_ref, *feats_refs):
    for tile in range(BLOCKS // 2):
        feats_ref = feats_refs[tile % len(feats_refs)]
        for block in (2 * tile, 2 * tile + 1):
            source = source_ref[block]
            tok_ref[block] = source.astype(BF16)
            src_ref[block] = source.T.astype(BF16)
        xt = jnp.concatenate([src_ref[2 * tile, :HD], src_ref[2 * tile + 1, :HD]], axis=1)
        write_features(xt.astype(F32), 1.0, feats_ref)
        tok = jnp.concatenate([tok_ref[2 * tile], tok_ref[2 * tile + 1]], axis=0)
        values = tok[:, HD:]
        zeros = jnp.zeros_like(values)
        part = dot(feats_ref[:HALF, :], jnp.concatenate([values, zeros], axis=1)) + dot(
            feats_ref[HALF:, :], jnp.concatenate([zeros, values], axis=1)
        )
        state_ref[...] = part if tile == 0 else state_ref[...] + part


def local_body(tiles, first_tile, tok_ref, src_ref, target_ref, local_ref, *out_refs):
    core = lax.axis_index("core")
    width = 2 * TB
    sign = 1 - 2 * core
    out_ref = target_ref
    if out_refs:
        out_ref = out_refs[0]
        for block in range(BLOCKS):
            out_ref[block] = target_ref[block].T.astype(BF16)
    local_ref[...] = jnp.zeros_like(local_ref)
    ahead = lax.broadcasted_iota(jnp.int32, (width, width), 0) - lax.broadcasted_iota(
        jnp.int32, (width, width), 1
    )

    def outer(number, carry):
        tile = first_tile + number
        target = jnp.concatenate([out_ref[2 * tile], out_ref[2 * tile + 1]], axis=1)
        zeros = jnp.zeros((HD, width), BF16)
        score_rhs = jnp.concatenate([target[:HD], zeros], axis=0)
        value_rhs = jnp.concatenate([zeros, target[HD:]], axis=0)

        def inner(source, carry):
            tok = jnp.concatenate([tok_ref[2 * source], tok_ref[2 * source + 1]], axis=0)
            scores = dot(tok, score_rhs)
            products = dot(tok, value_rhs)
            keep = (ahead + (source - tile) * width) * sign <= 0
            scaled = jnp.where(keep, scores, 0.0) * (1.0 / HD)
            attn = (scaled * scaled).astype(BF16)
            pgrad = (scaled * products * (2.0 / HD)).astype(BF16)
            left = jnp.concatenate([src_ref[2 * source], src_ref[2 * source + 1]], axis=1)
            local_ref[number, :HD] += dot(left[:HD], pgrad)
            local_ref[number, HD:] += dot(left[HD:], attn)
            return carry

        first = jnp.where(core == 0, 0, tile)
        last = jnp.where(core == 0, tile + 1, BLOCKS // 2)
        lax.fori_loop(first, last, inner, 0)
        return carry

    lax.fori_loop(0, tiles, outer, 0)


def scan_body(parts_ref, unused_ref, sums_ref):
    core = lax.axis_index("core")
    count = parts_ref.shape[0]
    cols, rows = lax.axis_size("zg"), lax.axis_size("x")

    def step(number, total):
        segment = number + core * (count - 1 - 2 * number)
        place = lax.rem(segment, cols) * rows + lax.div(segment, cols)
        sums_ref[place] = total
        return total + parts_ref[place]

    lax.fori_loop(0, count, step, jnp.zeros(parts_ref.shape[1:], F32))


def grads_body(state_ref, out_ref, early_ref, late_ref, grads_ref, rows_ref, cols_ref, *tile_refs):
    rows_ref[...] = state_ref[...].astype(BF16)
    for start in range(0, HALF, TB):
        stop = min(start + TB, HALF)
        part = state_ref[start:stop, :]
        if stop - start < TB:
            part = jnp.concatenate([part, jnp.zeros((TB - stop + start, TB), F32)], axis=0)
        cols_ref[:, start:stop] = part.T[:, : stop - start].astype(BF16)
    zeros = jnp.zeros((HD, 2 * TB), BF16)
    for tile in range(BLOCKS // 2):
        wide_ref, feats_ref = tile_refs[tile % 2], tile_refs[2 + tile % 2]
        target = jnp.concatenate([out_ref[2 * tile], out_ref[2 * tile + 1]], axis=1)
        wide_ref[:HALF] = dot(rows_ref[...], jnp.concatenate([target[HD:], zeros], axis=0))
        wide_ref[HALF:] = dot(rows_ref[...], jnp.concatenate([zeros, target[HD:]], axis=0))
        xt = target[:HD].astype(F32)
        write_features(xt, 2.0, feats_ref)
        values = dot(cols_ref[:HD, :], feats_ref[:HALF]) + dot(cols_ref[HD:, :], feats_ref[HALF:])
        back = chain_back(xt, wide_ref)
        local = early_ref[tile] if tile < 2 else late_ref[tile - 2]
        result = local + jnp.concatenate(
            [back * (2.0 / (HD * HD)), values * (1.0 / (HD * HD))], axis=0
        )
        grads_ref[2 * tile] = result[:, :TB].T
        grads_ref[2 * tile + 1] = result[:, TB:].T


def project_body(grads_ref, wq_ref, wk_ref, wv_ref, out_ref):
    query = jnp.concatenate([grads_ref[2 * h][:, :HD] for h in range(CHIPS)], axis=1)
    key = jnp.concatenate([grads_ref[2 * h + 1][:, :HD] for h in range(CHIPS)], axis=1)
    value = jnp.concatenate([grads_ref[2 * h + 1][:, HD:] for h in range(CHIPS)], axis=1)
    query, key, value = query.astype(BF16), key.astype(BF16), value.astype(BF16)
    width = out_ref.shape[2]
    for place in range(out_ref.shape[0]):
        cols = slice(place * width, (place + 1) * width)
        out_ref[place] = (
            dot(query, wq_ref[:, cols]) + dot(key, wk_ref[:, cols]) + dot(value, wv_ref[:, cols])
        )


def on_device(queries, keys, values, out_grad, w_query, w_key, w_value):
    shape = jax.ShapeDtypeStruct
    groups = lax.axis_size("x") * lax.axis_size("zg")
    packed = call(
        pack_body,
        shape((BLOCKS, TB, TB), F32),
        (queries, keys, values, out_grad),
        "pack",
        limit=None,
        flops=1 << 20,
        nbytes=1 << 20,
    )
    source = lax.all_to_all(packed, ("zc", "core"), 0, 0, tiled=True)
    target = lax.ppermute(source, "core", [(0, 1), (1, 0)])
    blocks = shape((BLOCKS, TB, TB), BF16)
    state, tok, src = call(
        state_body,
        (shape((HALF, TB), F32), blocks, blocks),
        (source,),
        "state",
        scratch=[pltpu.VMEM((2 * HALF, 2 * TB), BF16)] * 2,
        flops=4 << 30,
        nbytes=3 << 20,
    )
    parts = lax.all_to_all(
        state.reshape(groups, 1, HALF * TB // groups), ("zg", "x"), 0, 0, tiled=True
    )
    tiles = BLOCKS // 4
    halves = shape((tiles, TB, 2 * TB), F32)
    early, out = call(
        functools.partial(local_body, tiles, 0),
        (halves, blocks),
        (tok, src, target),
        "early",
        flops=2 << 30,
        nbytes=1 << 20,
    )
    sums = call(
        scan_body, shape(parts.shape, F32), (parts, early), "scan", flops=1 << 20, nbytes=1 << 20
    )
    before = lax.all_to_all(sums, ("zg", "x"), 0, 0, tiled=True).reshape(HALF, TB)
    (late,) = call(
        functools.partial(local_body, tiles, tiles),
        (halves,),
        (tok, src, out),
        "late",
        flops=2 << 30,
        nbytes=1 << 20,
    )
    grads = call(
        grads_body,
        shape((BLOCKS, TB, TB), F32),
        (before, out, early, late),
        "grads",
        scratch=[
            pltpu.VMEM((HALF, TB), BF16),
            pltpu.VMEM((TB, HALF), BF16),
            pltpu.VMEM((2 * HALF, 2 * TB), F32),
            pltpu.VMEM((2 * HALF, 2 * TB), F32),
            pltpu.VMEM((2 * HALF, 2 * TB), BF16),
            pltpu.VMEM((2 * HALF, 2 * TB), BF16),
        ],
        flops=4 << 30,
        nbytes=3 << 20,
    )
    mine = lax.all_to_all(grads, ("zc", "core"), 0, 0, tiled=True)
    heads = lax.axis_size("y")
    partial_sum = call(
        project_body,
        shape((heads, TB, w_query.shape[1] // heads), F32),
        (mine, w_query, w_key, w_value),
        "project",
        flops=1 << 29,
        nbytes=4 << 20,
    )
    pieces = lax.all_to_all(partial_sum, "y", 0, 0, tiled=True)
    return jnp.sum(pieces, axis=0).astype(BF16)


def solution(mesh):
    seq, head = mesh.devices.shape
    cols = 4 if seq >= 128 else 2
    grid = Mesh(
        mesh.devices.reshape(seq // (cols * 8), cols, CHIPS, 2, head),
        ("x", "zg", "zc", "core", "y"),
    )
    tokens = ("x", "zg", "zc", "core")
    placed = (P(tokens, "y"),) * 4 + (P("y", None),) * 3
    return jax.shard_map(
        on_device, mesh=grid, in_specs=placed, out_specs=P(tokens, "y"), check_vma=False
    )
```

```python
import functools

import jax
import jax.numpy as jnp
from jax import lax
from jax.experimental import pallas as pl
from jax.experimental.pallas import tpu as pltpu
from jax.sharding import Mesh
from jax.sharding import PartitionSpec as P

HD = 64
TB = 128
CHIPS = 4
BLOCKS = 8
GRAIN = 8
GRAINS = HD // GRAIN
HALF = 1040


def row_tiles():
    off = [
        [("off", j, other) for j in range(GRAIN * block, GRAIN * (block + 1)) for other in range(block + 1, GRAINS)]
        for block in range(GRAINS)
    ]
    ring = [[("ring", block, step) for step in range(GRAIN // 2)] for block in range(GRAINS)]
    left = [("left", block, block + 1) for block in range(0, GRAINS, 2)]
    first = off[0] + off[1] + sum(ring[:6], []) + left[:2]
    return first + sum(off[2:], []) + sum(ring[6:], []) + left[2:]


TILES = row_tiles()
assert len(TILES) * GRAIN == 2 * HALF
VMEM = pl.BlockSpec(memory_space=pltpu.VMEM)
F32 = jnp.float32
BF16 = jnp.bfloat16


def call(body, out_shape, args, name, scratch=(), flops=0, nbytes=0, limit=24 << 20):
    return pl.pallas_call(
        body,
        out_shape=out_shape,
        in_specs=[VMEM] * len(args),
        out_specs=jax.tree.map(lambda unused: VMEM, out_shape),
        scratch_shapes=list(scratch),
        name=name,
        compiler_params=pltpu.CompilerParams(vmem_limit_bytes=limit),
        cost_estimate=pl.CostEstimate(flops=flops, bytes_accessed=nbytes, transcendentals=0),
    )(*args)


def dot(a, b):
    return jnp.dot(a, b, preferred_element_type=F32)


def pack_body(q_ref, k_ref, v_ref, g_ref, out_ref):
    for head in range(CHIPS):
        cols = slice(head * HD, (head + 1) * HD)
        out_ref[2 * head] = jnp.concatenate([k_ref[:, cols], v_ref[:, cols]], axis=1).astype(F32)
        out_ref[2 * head + 1] = jnp.concatenate([q_ref[:, cols], g_ref[:, cols]], axis=1).astype(F32)


def turned(grain, step):
    return jnp.concatenate([grain[step:], grain[:step]], axis=0) if step else grain


def write_features(xt, factor, feats_ref):
    grains = [xt[GRAIN * block : GRAIN * (block + 1)] for block in range(GRAINS)]
    twice = [grain * factor for grain in grains] if factor != 1.0 else grains
    half = GRAIN // 2
    tiles = []
    for kind, one, two in TILES:
        if kind == "off":
            tiles.append(xt[one : one + 1] * twice[two])
        elif kind == "ring":
            tiles.append(grains[one] * turned(twice[one] if two else grains[one], two))
        else:
            pieces = [grains[block][:half] * twice[block][half:] for block in (one, two)]
            tiles.append(jnp.concatenate(pieces, axis=0))
    for place in range(0, len(tiles), 2):
        rows = slice(GRAIN * place, GRAIN * (place + 2))
        feats_ref[rows, :] = jnp.concatenate(tiles[place : place + 2], axis=0).astype(BF16)


def chain_back(xt, wide_ref):
    grains = [xt[GRAIN * block : GRAIN * (block + 1)] for block in range(GRAINS)]
    sums = [jnp.zeros(grains[0].shape, F32) for unused in range(GRAINS)]
    across = {}
    half = GRAIN // 2
    for place, (kind, one, two) in enumerate(TILES):
        wide = wide_ref[GRAIN * place : GRAIN * (place + 1)]
        if kind == "off":
            sums[two] = sums[two] + xt[one : one + 1] * wide
            term = grains[two] * wide
            across[one] = across[one] + term if one in across else term
        elif kind == "ring":
            sums[one] = sums[one] + turned(grains[one], two) * wide
            if two:
                sums[one] = sums[one] + turned(grains[one] * wide, GRAIN - two)
        else:
            for number, block in enumerate((one, two)):
                piece = wide[half * number : half * (number + 1)]
                term = [grains[block][half:] * piece, grains[block][:half] * piece]
                sums[block] = sums[block] + jnp.concatenate(term, axis=0)
    for block in range(GRAINS - 1):
        rows = [
            jnp.sum(across[j], axis=0, keepdims=True)
            for j in range(GRAIN * block, GRAIN * (block + 1))
        ]
        sums[block] = sums[block] + jnp.concatenate(rows, axis=0)
    return jnp.concatenate(sums, axis=0)


def state_body(source_ref, state_ref, tok_ref, src_ref, *feats_refs):
    for tile in range(BLOCKS // 2):
        feats_ref = feats_refs[tile % len(feats_refs)]
        for block in (2 * tile, 2 * tile + 1):
            source = source_ref[block]
            tok_ref[block] = source.astype(BF16)
            src_ref[block] = source.T.astype(BF16)
        xt = jnp.concatenate([src_ref[2 * tile, :HD], src_ref[2 * tile + 1, :HD]], axis=1)
        write_features(xt.astype(F32), 1.0, feats_ref)
        tok = jnp.concatenate([tok_ref[2 * tile], tok_ref[2 * tile + 1]], axis=0)
        values = tok[:, HD:]
        zeros = jnp.zeros_like(values)
        part = dot(feats_ref[:HALF, :], jnp.concatenate([values, zeros], axis=1)) + dot(
            feats_ref[HALF:, :], jnp.concatenate([zeros, values], axis=1)
        )
        state_ref[...] = part if tile == 0 else state_ref[...] + part


def local_body(tok_ref, src_ref, target_ref, local_ref, out_ref):
    core = lax.axis_index("core")
    tiles = BLOCKS // 2
    width = 2 * TB
    sign = 1 - 2 * core
    for block in range(BLOCKS):
        out_ref[block] = target_ref[block].T.astype(BF16)
    local_ref[...] = jnp.zeros_like(local_ref)
    ahead = lax.broadcasted_iota(jnp.int32, (width, width), 0) - lax.broadcasted_iota(
        jnp.int32, (width, width), 1
    )

    def outer(tile, carry):
        target = jnp.concatenate([out_ref[2 * tile], out_ref[2 * tile + 1]], axis=1)
        zeros = jnp.zeros((HD, width), BF16)
        score_rhs = jnp.concatenate([target[:HD], zeros], axis=0)
        value_rhs = jnp.concatenate([zeros, target[HD:]], axis=0)

        def inner(source, carry):
            tok = jnp.concatenate([tok_ref[2 * source], tok_ref[2 * source + 1]], axis=0)
            scores = dot(tok, score_rhs)
            products = dot(tok, value_rhs)
            keep = (ahead + (source - tile) * width) * sign <= 0
            scaled = jnp.where(keep, scores, 0.0) * (1.0 / HD)
            attn = (scaled * scaled).astype(BF16)
            pgrad = (scaled * products * (2.0 / HD)).astype(BF16)
            left = jnp.concatenate([src_ref[2 * source], src_ref[2 * source + 1]], axis=1)
            local_ref[tile, :HD] += dot(left[:HD], pgrad)
            local_ref[tile, HD:] += dot(left[HD:], attn)
            return carry

        first = jnp.where(core == 0, 0, tile)
        last = jnp.where(core == 0, tile + 1, tiles)
        lax.fori_loop(first, last, inner, 0)
        return carry

    lax.fori_loop(0, tiles, outer, 0)


def scan_body(parts_ref, sums_ref):
    core = lax.axis_index("core")
    count = parts_ref.shape[0]
    cols, rows = lax.axis_size("zg"), lax.axis_size("x")

    def step(number, total):
        segment = number + core * (count - 1 - 2 * number)
        place = lax.rem(segment, cols) * rows + lax.div(segment, cols)
        sums_ref[place] = total
        return total + parts_ref[place]

    lax.fori_loop(0, count, step, jnp.zeros(parts_ref.shape[1:], F32), unroll=True)


def grads_body(state_ref, out_ref, local_ref, grads_ref, rows_ref, cols_ref, *tile_refs):
    rows_ref[...] = state_ref[...].astype(BF16)
    for start in range(0, HALF, TB):
        stop = min(start + TB, HALF)
        part = state_ref[start:stop, :]
        if stop - start < TB:
            part = jnp.concatenate([part, jnp.zeros((TB - stop + start, TB), F32)], axis=0)
        cols_ref[:, start:stop] = part.T[:, : stop - start].astype(BF16)
    zeros = jnp.zeros((HD, 2 * TB), BF16)
    for tile in range(BLOCKS // 2):
        wide_ref, feats_ref = tile_refs[tile % 2], tile_refs[2 + tile % 2]
        target = jnp.concatenate([out_ref[2 * tile], out_ref[2 * tile + 1]], axis=1)
        wide_ref[:HALF] = dot(rows_ref[...], jnp.concatenate([target[HD:], zeros], axis=0))
        wide_ref[HALF:] = dot(rows_ref[...], jnp.concatenate([zeros, target[HD:]], axis=0))
        xt = target[:HD].astype(F32)
        write_features(xt, 2.0, feats_ref)
        values = dot(cols_ref[:HD, :], feats_ref[:HALF]) + dot(cols_ref[HD:, :], feats_ref[HALF:])
        back = chain_back(xt, wide_ref)
        result = local_ref[tile] + jnp.concatenate(
            [back * (2.0 / (HD * HD)), values * (1.0 / (HD * HD))], axis=0
        )
        grads_ref[2 * tile] = result[:, :TB].T
        grads_ref[2 * tile + 1] = result[:, TB:].T


def project_body(grads_ref, wq_ref, wk_ref, wv_ref, out_ref):
    query = jnp.concatenate([grads_ref[2 * h][:, :HD] for h in range(CHIPS)], axis=1)
    key = jnp.concatenate([grads_ref[2 * h + 1][:, :HD] for h in range(CHIPS)], axis=1)
    value = jnp.concatenate([grads_ref[2 * h + 1][:, HD:] for h in range(CHIPS)], axis=1)
    query, key, value = query.astype(BF16), key.astype(BF16), value.astype(BF16)
    width = out_ref.shape[2]
    for place in range(out_ref.shape[0]):
        cols = slice(place * width, (place + 1) * width)
        out_ref[place] = (
            dot(query, wq_ref[:, cols]) + dot(key, wk_ref[:, cols]) + dot(value, wv_ref[:, cols])
        )


def on_device(queries, keys, values, out_grad, w_query, w_key, w_value):
    shape = jax.ShapeDtypeStruct
    groups = lax.axis_size("x") * lax.axis_size("zg")
    packed = call(
        pack_body,
        shape((BLOCKS, TB, TB), F32),
        (queries, keys, values, out_grad),
        "pack",
        limit=None,
        flops=1 << 20,
        nbytes=1 << 20,
    )
    source = lax.all_to_all(packed, ("zc", "core"), 0, 0, tiled=True)
    target = lax.ppermute(source, "core", [(0, 1), (1, 0)])
    blocks = shape((BLOCKS, TB, TB), BF16)
    state, tok, src = call(
        state_body,
        (shape((HALF, TB), F32), blocks, blocks),
        (source,),
        "state",
        scratch=[pltpu.VMEM((2 * HALF, 2 * TB), BF16)] * 2,
        flops=4 << 30,
        nbytes=3 << 20,
    )
    parts = lax.all_to_all(
        state.reshape(groups, 1, HALF * TB // groups), ("zg", "x"), 0, 0, tiled=True
    )
    sums = call(
        scan_body, shape(parts.shape, F32), (parts,), "scan", flops=1 << 20, nbytes=1 << 20
    )
    before = lax.all_to_all(sums, ("zg", "x"), 0, 0, tiled=True).reshape(HALF, TB)
    local, out = call(
        local_body,
        (shape((BLOCKS // 2, TB, 2 * TB), F32), blocks),
        (tok, src, target),
        "local",
        flops=4 << 30,
        nbytes=1 << 20,
    )
    grads = call(
        grads_body,
        shape((BLOCKS, TB, TB), F32),
        (before, out, local),
        "grads",
        scratch=[
            pltpu.VMEM((HALF, TB), BF16),
            pltpu.VMEM((TB, HALF), BF16),
            pltpu.VMEM((2 * HALF, 2 * TB), F32),
            pltpu.VMEM((2 * HALF, 2 * TB), F32),
            pltpu.VMEM((2 * HALF, 2 * TB), BF16),
            pltpu.VMEM((2 * HALF, 2 * TB), BF16),
        ],
        flops=4 << 30,
        nbytes=3 << 20,
    )
    mine = lax.all_to_all(grads, ("zc", "core"), 0, 0, tiled=True)
    heads = lax.axis_size("y")
    partial_sum = call(
        project_body,
        shape((heads, TB, w_query.shape[1] // heads), F32),
        (mine, w_query, w_key, w_value),
        "project",
        flops=1 << 29,
        nbytes=4 << 20,
    )
    pieces = lax.all_to_all(partial_sum, "y", 0, 0, tiled=True)
    return jnp.sum(pieces, axis=0).astype(BF16)


def solution(mesh):
    seq, head = mesh.devices.shape
    cols = 4 if seq >= 128 else 2
    grid = Mesh(
        mesh.devices.reshape(seq // (cols * 8), cols, CHIPS, 2, head),
        ("x", "zg", "zc", "core", "y"),
    )
    tokens = ("x", "zg", "zc", "core")
    placed = (P(tokens, "y"),) * 4 + (P("y", None),) * 3
    return jax.shard_map(
        on_device, mesh=grid, in_specs=placed, out_specs=P(tokens, "y"), check_vma=False
    )
```
